32 devices in a mesh: groups: 2 (over y), seq: 4 (over z), exp: 2 (over x), tp: 2 (over core).
Axes of the slice: x: 2, y: 2, z: 4, core: 2. Of those that a mesh axis runs over, the one named last changes fastest.
Arguments:
- attn_query: bfloat16 [2048, 1152], P(('groups', 'seq'), ('exp', 'tp')), parts along dimension 0, may hold values from -6 to 6
- fresh_keys: bfloat16 [2048, 1152], P(('groups', 'seq'), ('exp', 'tp')), parts along dimension 0, may hold values from -6 to 6
- fresh_values: bfloat16 [2048, 1152], P(('groups', 'seq'), ('exp', 'tp')), parts along dimension 0, may hold values from -6 to 6
- stale_keys: bfloat16 [2048, 1152], P(('groups', 'seq'), ('exp', 'tp')), parts along dimension 0, may hold values from -6 to 6
- stale_values: bfloat16 [2048, 1152], P(('groups', 'seq'), ('exp', 'tp')), parts along dimension 0, may hold values from -6 to 6
- block_flags: int32 [16], P(('groups', 'seq')), parts along dimension 0, may hold values 0 or 1
- moe_tokens: bfloat16 [4096, 1152], P(('groups', 'seq', 'exp', 'tp')), parts along dimension 0, may hold values from -6 to 6
- expert_ids: int32 [4096, 2], P(('groups', 'seq', 'exp', 'tp')), parts along dimension 0, may hold values from 0 to 3, all different within a row; in each aligned block of 128 rows (0 to 127, 128 to 255, ...) at most 80 rows name the same one
- gate_weights: float32 [4096, 2], P(('groups', 'seq', 'exp', 'tp')), parts along dimension 0, may hold values from 0.25 to 1
- up_weight: bfloat16 [4, 1152, 4608], P('seq', None, ('exp', 'tp')), may hold values from -0.1875 to 0.1875
- up_bias: float32 [4, 4608], P('seq', ('exp', 'tp')), may hold values from -3 to 3
- down_weight: bfloat16 [4, 4608, 1152], P('seq', ('exp', 'tp')), may hold values from -0.09375 to 0.09375
- down_bias: float32 [4, 1152], P('seq'), may hold values from -2 to 2
Outputs:
- attn_out: bfloat16 [2048, 1152], P(('groups', 'seq'), ('exp', 'tp')), parts along dimension 0
- moe_out: bfloat16 [4096, 1152], P(('groups', 'seq', 'exp', 'tp')), parts along dimension 0
The draws below stay inside these ranges and needn't reach their ends.
There are 2 independent parts, one for each index of `groups`. The reference program is written for one: setup_inputs(seed, part) draws one part's arguments, and reference() takes and returns one part's arrays. A program takes and returns all parts, laid end to end along the dimension named above; an argument that names none is the same for every part. Nothing has to cross between parts.
Inputs may be any that keep to these rules, and one draw needn't show every extreme that they name: `expert_ids`: the 2 ids of a token differ. In the rows of one device no expert is named more than 80 times, and in every draw some expert is named exactly 80 times in some device's rows.
All inputs are finite; a program needn't handle non-finite values. No bound on the sum of `block_flags` on one device may be relied on, other than what follows from the above.
Results may differ from the reference program's by a relative error of at most 0.014.
Values may be sent and summed in bfloat16 or wider, within the bound.
A program may use at most 64 MiB of HBM per device.

```python
import math
import jax
import jax.numpy as jnp
import numpy as np
from jax import lax

D = 1152
HEADS = 16
HD = 72
FF = 4608
TOP = 2
EXPERTS = 4
BLK = 128
TOK_DEV = 128
SEQLEN = 1024
MOE_TOK = 2048
CAP = 80


def drawn(key):
    shape = (SEQLEN, HEADS * HD)
    query = jnp.clip(jax.random.normal(jax.random.fold_in(key, 101), shape, jnp.float32), -6.0, 6.0)
    keys_new = jnp.clip(jax.random.normal(jax.random.fold_in(key, 102), shape, jnp.float32), -6.0, 6.0)
    keys_old = jnp.clip(jax.random.normal(jax.random.fold_in(key, 103), shape, jnp.float32), -6.0, 6.0)
    return (query, keys_new, keys_old)


def draw_attn_query(key, part):
    return drawn(key)[0].astype(jnp.bfloat16)


def draw_fresh_keys(key, part):
    return drawn(key)[1].astype(jnp.bfloat16)


def draw_stale_keys(key, part):
    return drawn(key)[2].astype(jnp.bfloat16)


def place_ends(values, key, smallest, high):
    spot = [jax.random.randint(jax.random.fold_in(key, axis), (), 0, length) for axis, length in enumerate(values.shape)]
    main_axis = values.shape.index(max(values.shape))
    neighbour = spot[:main_axis] + [(spot[main_axis] + 1) % values.shape[main_axis]] + spot[main_axis + 1:]
    return values.at[tuple(spot)].set(smallest).at[tuple(neighbour)].set(high)


def steps_of(key, dims, shards, smallest, top_value):
    level = 1.0
    for dim, blocks in shards:
        heights = jax.random.uniform(jax.random.fold_in(jax.random.fold_in(key, 6), dim), (blocks,), jnp.float32, smallest / len(shards), top_value / len(shards))
        level = level * jnp.repeat(jnp.exp(heights), dims[dim] // blocks).reshape((-1,) + (1,) * (len(dims) - 1 - dim))
    return level


def assign_block(rng, own, number, rows, number_of, top, limit, lean):
    ranking = jax.random.permutation(rng, number_of)
    heavy_load, ordinary = portions_of(number_of, rows * top, limit, lean, True), portions_of(number_of, rows * top, limit, lean, False)
    places = jnp.arange(number_of)

    def named(tallies, offset_by):
        used = int((tallies > 0).sum())
        fixed = max(1, used // 4)
        passed = fixed + (places - fixed + offset_by * (used - fixed)) % max(1, number_of - fixed)
        return jnp.zeros((number_of,), jnp.int32).at[ranking[jnp.where(places < fixed, places, passed)]].set(jnp.asarray(tallies, jnp.int32))

    tallies = jnp.where(number % 4 == 0, named(heavy_load, number // 4), named(ordinary, number - number // 4 - 1))
    mixed = jax.random.permutation(jax.random.fold_in(own, 3), number_of)
    giver, sink = mixed[0:number_of // 2 * 2:2], mixed[1:number_of // 2 * 2:2]
    slack = jnp.minimum(tallies[giver] - 1, limit - tallies[sink]) // 2
    slack = jnp.where((giver == ranking[0]) | (sink == ranking[0]) | (tallies[sink] == 0), 0, jnp.maximum(slack, 0))
    passed = jax.random.randint(jax.random.fold_in(own, 4), (number_of // 2,), 0, 1 << 20) % (slack + 1)
    tallies = tallies.at[giver].add(-passed).at[sink].add(passed)
    labels = jnp.searchsorted(jnp.cumsum(tallies), jnp.arange(rows * top), side="right").astype(jnp.int32)
    listing = labels.reshape(top, rows).T
    listing = listing[jax.random.permutation(jax.random.fold_in(own, 1), rows)]
    offset_by = jax.random.randint(jax.random.fold_in(own, 2), (rows, 1), 0, top)
    return jnp.take_along_axis(listing, (jnp.arange(top)[None, :] + offset_by) % top, axis=1)


def portions_of(amount, total, limit, lean, full):
    weights = [(1 << 20) // math.isqrt(grade ** lean) + 1 for grade in range(1, amount + 1)]
    largest = limit if full else min(limit, max(-(-total // amount), total * weights[0] // sum(weights)))
    least = 1 if total - largest >= amount - 1 else 0
    given, spare = [largest] + [least] * (amount - 1), total - largest - least * (amount - 1)
    while spare > 0:
        free = [i for i in range(1, amount) if given[i] < largest] or [i for i in range(1, amount) if given[i] < limit]
        whole, budget = sum([weights[i] for i in free]), spare
        for i in free:
            more = min(limit - given[i], max(1, budget * weights[i] // whole), spare)
            given[i] = given[i] + more
            spare = spare - more
    return np.array(given)


def noise(key, dims, width, limit, cuts=(), kind=jnp.bfloat16):
    values = jax.random.normal(key, dims, jnp.float32) * width
    if len(cuts) > 0:
        values = steps_of(key, dims, cuts, -0.22, 0.18) * values
    return jnp.clip(values, min=-limit, max=limit).astype(kind)


def setup_inputs(seed: int = 0, part: int = 0) -> dict:
    streams_of = jax.random.split(jax.random.key(seed), 14)
    part_splits = jax.random.split(jax.random.fold_in(streams_of[13], part), 14)
    attn_query = draw_attn_query(jax.random.fold_in(jax.random.fold_in(streams_of[13], part), 71), part)
    fresh_keys = draw_fresh_keys(jax.random.fold_in(jax.random.fold_in(streams_of[13], part), 71), part)
    fresh_values = noise(part_splits[2], (SEQLEN, HEADS * HD), 1.0, 6.0, ((0, 4), (1, 4)))
    stale_keys = draw_stale_keys(jax.random.fold_in(jax.random.fold_in(streams_of[13], part), 71), part)
    stale_values = noise(part_splits[4], (SEQLEN, HEADS * HD), 1.0, 6.0, ((0, 4), (1, 4)))
    block_flags = place_ends((jax.random.randint(part_splits[5], (SEQLEN // BLK,), 0, 2) < 1).astype(jnp.int32), jax.random.fold_in(part_splits[5], 1), 0, 1)
    moe_tokens = noise(part_splits[6], (MOE_TOK, D), 1.0, 6.0, ((0, 16),))
    expert_ids_keys = jax.random.split(jax.random.fold_in(part_splits[7], 1), MOE_TOK // TOK_DEV)
    expert_ids_turns = jax.random.permutation(jax.random.fold_in(part_splits[7], 3), MOE_TOK // TOK_DEV)
    expert_ids = jax.vmap(lambda own, number: assign_block(jax.random.fold_in(part_splits[7], 2), own, number, TOK_DEV, EXPERTS, TOP, CAP, 2))(expert_ids_keys, expert_ids_turns).reshape((MOE_TOK, TOP))
    gate_weights = jnp.clip(jnp.exp(math.log(1.0) - 1.3862944 * jax.random.uniform(part_splits[8], (MOE_TOK, TOP), jnp.float32) ** steps_of(part_splits[8], (MOE_TOK, TOP), ((0, 16),), -0.2, 0.2)), 0.25, 1.0)
    up_weight = noise(streams_of[9], (EXPERTS, D, FF), D ** -0.5, 0.1875, ((0, 4), (2, 4)))
    up_bias = noise(streams_of[10], (EXPERTS, FF), 0.5, 3.0, ((0, 4), (1, 4)), jnp.float32)
    down_weight = noise(streams_of[11], (EXPERTS, FF, D), FF ** -0.5, 0.09375, ((0, 4), (1, 4)))
    down_bias = noise(streams_of[12], (EXPERTS, D), 0.3, 2.0, ((0, 4),), jnp.float32)
    return {"attn_query": attn_query, "fresh_keys": fresh_keys, "fresh_values": fresh_values, "stale_keys": stale_keys, "stale_values": stale_values, "block_flags": block_flags, "moe_tokens": moe_tokens, "expert_ids": expert_ids, "gate_weights": gate_weights, "up_weight": up_weight, "up_bias": up_bias, "down_weight": down_weight, "down_bias": down_bias}


def attention_part(attn_query, fresh_keys, fresh_values, stale_keys, stale_values, block_flags):
    row_flags = (jnp.repeat(block_flags, BLK) == 1)[:, None]
    keys = jnp.where(row_flags, fresh_keys, stale_keys)
    values = jnp.where(row_flags, fresh_values, stale_values)
    scale = 1.0 / math.sqrt(HD)
    query_block = math.gcd(SEQLEN, 1024)

    def head_fn(head):
        first = (head * HD).astype(jnp.int32)
        head_query = lax.dynamic_slice_in_dim(attn_query, first, HD, 1)
        head_keys = lax.dynamic_slice_in_dim(keys, first, HD, 1)
        head_values = lax.dynamic_slice_in_dim(values, first, HD, 1)

        def block_fn(index):
            lead = (index * query_block).astype(jnp.int32)
            rows = lax.dynamic_slice_in_dim(head_query, lead, query_block, 0)
            scores = jnp.dot(rows, head_keys.T, preferred_element_type=jnp.float32) * scale
            highest = lax.optimization_barrier(jnp.max(scores, axis=-1, keepdims=True))
            probs = jnp.exp(scores - highest)
            totals = lax.optimization_barrier(jnp.sum(probs, axis=-1, keepdims=True))
            mixed = jnp.dot(probs.astype(jnp.bfloat16), head_values, preferred_element_type=jnp.float32) / totals
            return mixed.astype(jnp.bfloat16)
        return lax.map(block_fn, jnp.arange(SEQLEN // query_block, dtype=jnp.int32))
    heads_out = lax.map(head_fn, jnp.arange(HEADS, dtype=jnp.int32))
    heads_out = heads_out.reshape(HEADS, SEQLEN, HD)
    return jnp.transpose(heads_out, (1, 0, 2)).reshape(SEQLEN, HEADS * HD)

def expert_part(moe_tokens, expert_ids, gate_weights, up_weight, up_bias, down_weight, down_bias):
    blocks = MOE_TOK // TOK_DEV
    block_ids = expert_ids.reshape(blocks, TOP * TOK_DEV)
    hits = (block_ids[:, :, None] == jnp.arange(EXPERTS, dtype=jnp.int32)[None, None, :]).astype(jnp.int32)
    before = jnp.cumsum(hits, axis=1) - hits
    place = lax.optimization_barrier(jnp.sum(before * hits, axis=-1)).reshape(-1).astype(jnp.int32)
    flat_expert = block_ids.reshape(-1).astype(jnp.int32)
    flat_block = jnp.repeat(jnp.arange(blocks, dtype=jnp.int32), TOP * TOK_DEV)
    repeated = jnp.repeat(moe_tokens, TOP, axis=0)
    buffer = jnp.zeros((EXPERTS, blocks, CAP, D), jnp.bfloat16)
    buffer = buffer.at[flat_expert, flat_block, place].set(repeated)

    def expert_fn(operands):
        slots, w_up, b_up, w_down, b_down = operands
        rows = slots.reshape(blocks * CAP, D)
        hidden = jax.nn.gelu(jnp.dot(rows, w_up, preferred_element_type=jnp.float32) + b_up[None, :]).astype(jnp.bfloat16)
        result = jnp.dot(hidden, w_down, preferred_element_type=jnp.float32) + b_down[None, :]
        return result.astype(jnp.bfloat16).reshape(blocks, CAP, D)
    expert_y = lax.map(expert_fn, (buffer, up_weight, up_bias, down_weight, down_bias))
    picked = expert_y[flat_expert, flat_block, place].reshape(MOE_TOK, TOP, D).astype(jnp.float32)
    combined = lax.optimization_barrier(jnp.sum(picked * gate_weights[:, :, None], axis=1))
    return combined.astype(jnp.bfloat16)

def reference(attn_query, fresh_keys, fresh_values, stale_keys, stale_values, block_flags, moe_tokens, expert_ids, gate_weights, up_weight, up_bias, down_weight, down_bias):
    attn_out = attention_part(attn_query, fresh_keys, fresh_values, stale_keys, stale_values, block_flags)
    moe_out = expert_part(moe_tokens, expert_ids, gate_weights, up_weight, up_bias, down_weight, down_bias)
    return (attn_out, moe_out)
```

```python
import math

import jax
import jax.numpy as jnp
from jax import lax
from jax.sharding import PartitionSpec as P

HD = 72


def attention_part(attn_query, fresh_keys, fresh_values, stale_keys, stale_values, block_flags):
    length = attn_query.shape[0]
    heads_here = attn_query.shape[1] // HD
    row_flags = (jnp.repeat(block_flags, length // block_flags.shape[0]) == 1)[:, None]
    keys = jnp.where(row_flags, fresh_keys, stale_keys)
    values = jnp.where(row_flags, fresh_values, stale_values)
    queries = attn_query.reshape(length, heads_here, HD)
    scale = 1.0 / math.sqrt(HD)
    initial = (
        jnp.full((heads_here, length), -1e30, jnp.float32),
        jnp.zeros((heads_here, length), jnp.float32),
        jnp.zeros((heads_here, length, HD), jnp.float32),
    )
    carry = initial
    both = lax.all_gather(jnp.concatenate([keys, values], axis=1), "seq", axis=0, tiled=True)
    piece = (both[:, : keys.shape[1]], both[:, keys.shape[1] :])
    count = piece[0].shape[0]
    width = math.gcd(count, 512)
    key_blocks = piece[0].reshape(count // width, width, heads_here, HD)
    value_blocks = piece[1].reshape(count // width, width, heads_here, HD)

    def advance(state, blocks):
        highest, totals, weighted = state
        key_block, value_block = blocks
        scores = (
            jnp.einsum("qhd,khd->hqk", queries, key_block, preferred_element_type=jnp.float32)
            * scale
        )
        new_high = jnp.maximum(highest, jnp.max(scores, axis=-1))
        rescale = jnp.exp(highest - new_high)
        probs = jnp.exp(scores - new_high[:, :, None])
        totals = totals * rescale + jnp.sum(probs, axis=-1)
        weighted = weighted * rescale[:, :, None] + jnp.einsum(
            "hqk,khd->hqd",
            probs.astype(jnp.bfloat16),
            value_block,
            preferred_element_type=jnp.float32,
        )
        return ((new_high, totals, weighted), None)

    carry, unused = lax.scan(advance, carry, (key_blocks, value_blocks))
    highest, totals, weighted = carry
    mixed = weighted / totals[:, :, None]
    return jnp.transpose(mixed, (1, 0, 2)).reshape(length, heads_here * HD).astype(jnp.bfloat16)


def expert_part(moe_tokens, expert_ids, gate_weights, up_weight, up_bias, down_weight, down_bias):
    tokens_here, width = moe_tokens.shape
    choose = expert_ids.shape[1]
    number = lax.axis_size("seq") * up_weight.shape[0]
    capacity = 5 * tokens_here // (2 * number)
    flat_ids = expert_ids.reshape(-1)
    hits = (flat_ids[:, None] == jnp.arange(number, dtype=jnp.int32)[None, :]).astype(jnp.int32)
    before = jnp.cumsum(hits, axis=0) - hits
    place = jnp.sum(before * hits, axis=1)
    slot = flat_ids * capacity + place
    slot_pairs = slot.reshape(tokens_here, choose)
    table = jnp.sum(
        (
            slot_pairs[None, :, :] == jnp.arange(number * capacity, dtype=jnp.int32)[:, None, None]
        ).astype(jnp.int32),
        axis=-1,
    )
    buffer = jnp.dot(
        table.astype(jnp.bfloat16), moe_tokens, preferred_element_type=jnp.float32
    ).astype(jnp.bfloat16)
    buffer = buffer.reshape(number, capacity, width)
    received = lax.all_to_all(buffer, "seq", split_axis=0, concat_axis=0, tiled=True)
    sources = received.shape[0]
    count = received.shape[1]
    flat_rows = received.reshape(sources * count, width)
    chip_rows = lax.all_gather(flat_rows, ("exp", "tp"), axis=0, tiled=True)
    hidden = jax.nn.gelu(
        jnp.dot(chip_rows, up_weight[0], preferred_element_type=jnp.float32) + up_bias
    ).astype(jnp.bfloat16)
    summed = lax.psum_scatter(
        jnp.dot(hidden, down_weight[0], preferred_element_type=jnp.float32).astype(jnp.bfloat16),
        ("exp", "tp"),
        scatter_dimension=0,
        tiled=True,
    ).astype(jnp.float32)
    result = (summed + down_bias[0][None, :]).astype(jnp.bfloat16).reshape(sources, count, width)
    returned = lax.all_to_all(result, "seq", split_axis=0, concat_axis=0, tiled=True)
    flat_out = returned.reshape(number * capacity, width)
    picked = flat_out[slot].reshape(tokens_here, choose, width).astype(jnp.float32)
    combined = jnp.sum(picked * gate_weights[:, :, None], axis=1)
    return combined.astype(jnp.bfloat16)


def local(
    attn_query,
    fresh_keys,
    fresh_values,
    stale_keys,
    stale_values,
    block_flags,
    moe_tokens,
    expert_ids,
    gate_weights,
    up_weight,
    up_bias,
    down_weight,
    down_bias,
):
    attn_out = attention_part(
        attn_query, fresh_keys, fresh_values, stale_keys, stale_values, block_flags
    )
    moe_out = expert_part(
        moe_tokens, expert_ids, gate_weights, up_weight, up_bias, down_weight, down_bias
    )
    return (attn_out, moe_out)


def solution(mesh):
    in_specs = (
        P(("groups", "seq"), ("exp", "tp")),
        P(("groups", "seq"), ("exp", "tp")),
        P(("groups", "seq"), ("exp", "tp")),
        P(("groups", "seq"), ("exp", "tp")),
        P(("groups", "seq"), ("exp", "tp")),
        P(("groups", "seq")),
        P(("groups", "seq", "exp", "tp"), None),
        P(("groups", "seq", "exp", "tp"), None),
        P(("groups", "seq", "exp", "tp"), None),
        P("seq", None, ("exp", "tp")),
        P("seq", ("exp", "tp")),
        P("seq", ("exp", "tp"), None),
        P("seq", None),
    )
    out_specs = (P(("groups", "seq"), ("exp", "tp")), P(("groups", "seq", "exp", "tp"), None))
    return jax.shard_map(local, mesh=mesh, in_specs=in_specs, out_specs=out_specs, check_vma=False)
```

```python
import functools
import math

import jax
import jax.numpy as jnp
from jax import lax
from jax.experimental import pallas as pl
from jax.experimental.pallas import tpu as pltpu
from jax.sharding import PartitionSpec as P

HD = 72
MESH = pl.DeviceIdType.MESH
F32 = jnp.float32
BF16 = jnp.bfloat16


def layer_kernel(
    sizes,
    q_ref, fresh_k, fresh_v, stale_k, stale_v, flags,
    tok_ref, ids_ref, idst_ref, gate_ref,
    up_hbm, upb_ref, down_hbm, downb_ref,
    attn_ref, moe_ref,
    up_v, down_v, place_v, disp, rows, tpin, xin, fin, ret, kv, acc,
    w_sem,
    z_send, z_recv, xf_send, xf_recv, tf_send, tf_recv,
    tr_send, tr_recv, xr_send, xr_recv, zr_send, zr_recv, kv_send, kv_recv,
):
    S, X, capp = sizes
    s, x, c = lax.axis_index("seq"), lax.axis_index("exp"), lax.axis_index("tp")
    oc = 1 - c
    T, D = tok_ref.shape
    L, W = q_ref.shape
    heads = W // HD
    blk = L // flags.shape[0]

    up_copy = pltpu.make_async_copy(up_hbm.at[0], up_v, w_sem.at[0])
    down_copy = pltpu.make_async_copy(down_hbm.at[0], down_v, w_sem.at[1])
    up_copy.start()
    down_copy.start()

    def rdma(src, dst, ssem, rsem, where):
        return pltpu.make_async_remote_copy(
            src_ref=src, dst_ref=dst, send_sem=ssem, recv_sem=rsem,
            device_id=where, device_id_type=MESH,
        )

    def z_copy(e, slot):
        return rdma(disp.at[e], rows.at[slot, c, x], z_send.at[e], z_recv.at[slot], {"seq": e})

    def x_forward(src, to, origin):
        return rdma(
            rows.at[src, c, origin], rows.at[src, c, origin],
            xf_send.at[src, to], xf_recv.at[src, origin], {"exp": to},
        )

    def t_forward(src, origin, side):
        return rdma(
            rows.at[src, side, origin], rows.at[src, side, origin],
            tf_send.at[src, origin], tf_recv.at[src, origin], {"tp": oc},
        )

    def t_reduce(src):
        return rdma(rows.at[src, oc], tpin.at[src], tr_send.at[src], tr_recv.at[src], {"tp": oc})

    def x_reduce(src, to, origin):
        return rdma(
            rows.at[src, c, to], xin.at[src, origin],
            xr_send.at[src, to], xr_recv.at[src, origin], {"exp": to},
        )

    def z_return(src, slot):
        return rdma(fin.at[src], ret.at[slot], zr_send.at[src], zr_recv.at[slot], {"seq": src})

    def kv_copy(to, slot):
        return rdma(kv.at[slot], kv.at[slot], kv_send.at[to], kv_recv.at[slot], {"seq": to})

    def other_x(i):
        return lax.rem(x + i, X)

    def order(k):
        half = (k + 1) // 2
        return lax.rem(s + half * (2 * lax.rem(k, 2) - 1) + S, S)

    barrier = pltpu.get_barrier_semaphore()
    for i in range(1, S):
        pl.semaphore_signal(barrier, inc=1, device_id={"seq": lax.rem(s + i, S)}, device_id_type=MESH)
    for i in range(1, X):
        pl.semaphore_signal(barrier, inc=1, device_id={"exp": other_x(i)}, device_id_type=MESH)
    pl.semaphore_signal(barrier, inc=1, device_id={"tp": oc}, device_id_type=MESH)

    expert = lax.broadcasted_iota(jnp.int32, (S, T), 0)
    named = (idst_ref[0:1, :] == expert) | (idst_ref[1:2, :] == expert)
    earlier = lax.broadcasted_iota(jnp.int32, (T, T), 0) < lax.broadcasted_iota(jnp.int32, (T, T), 1)
    place = jnp.dot(
        jnp.where(named, 1.0, 0.0).astype(BF16),
        jnp.where(earlier, 1.0, 0.0).astype(BF16),
        preferred_element_type=F32,
    )
    place_v[...] = jnp.where(named, place, -1.0)
    slot_rows = lax.broadcasted_iota(jnp.int32, (capp, T), 0).astype(F32)

    def slots_of(e):
        pick = jnp.where(place_v[pl.ds(e, 1), :] == slot_rows, 1.0, 0.0).astype(BF16)
        return jnp.dot(pick, tok_ref[...], preferred_element_type=F32).astype(BF16)

    def forward(src):
        for i in range(1, X):
            x_forward(src, other_x(i), x).start()
        t_forward(src, x, c).start()

    rows[s, c, x] = slots_of(s)
    pl.semaphore_wait(barrier, S - 1 + X - 1 + 1)
    forward(s)
    for k in range(1, S):
        e = order(k)
        disp[e] = slots_of(e)
        z_copy(e, s).start()

    for b in range(flags.shape[0]):
        fresh = flags[b] == 1
        part = pl.ds(b * blk, blk)
        kv[s, 0, part, :] = jnp.where(fresh, fresh_k[part, :], stale_k[part, :])
        kv[s, 1, part, :] = jnp.where(fresh, fresh_v[part, :], stale_v[part, :])
    for k in range(1, S):
        kv_copy(order(k), s).start()

    up_copy.wait()
    down_copy.wait()

    def finish(src):
        total = rows[src, c, x].astype(F32) + downb_ref[...]
        for i in range(1, X):
            x_reduce(src, other_x(i), other_x(i)).wait_recv()
            total = total + xin[src, other_x(i)].astype(F32)
        done = total.astype(BF16)
        fin[src] = done

    def finish_send(src):
        finish(src)

        @pl.when(src != s)
        def _():
            z_return(src, s).start()

        @pl.when(src == s)
        def _():
            ret[s] = fin[s]

    def chunk(k, unused):
        src = order(k)
        for i in range(1, X):
            x_forward(src, other_x(i), other_x(i)).wait_recv()
            t_forward(src, other_x(i), c).start()

        @pl.when(k + 1 < S)
        def _():
            nxt = order(k + 1)
            z_copy(nxt, nxt).wait_recv()
            forward(nxt)

        for i in range(X):
            t_forward(src, other_x(i), oc).wait_recv()
        for i in range(1, X):
            x_forward(src, other_x(i), x).wait_send()
        for i in range(X):
            t_forward(src, other_x(i), c).wait_send()

        block = rows[src].reshape(2 * X * capp, D)
        hidden = jnp.dot(block, up_v[...], preferred_element_type=F32) + upb_ref[...]
        hidden = jax.nn.gelu(hidden).astype(BF16)
        result = jnp.dot(hidden, down_v[...], preferred_element_type=F32).astype(BF16)
        rows[src] = result.reshape(2, X, capp, D)
        t_reduce(src).start()

        @pl.when(k >= 1)
        def _():
            finish_send(order(k - 1))

        t_reduce(src).wait_recv()
        for i in range(X):
            to = other_x(i)
            rows[src, c, to] = (rows[src, c, to].astype(F32) + tpin[src, to].astype(F32)).astype(BF16)
            if i > 0:
                x_reduce(src, to, x).start()
        return unused

    lax.fori_loop(0, S, chunk, jnp.int32(0))

    for i in range(1, S):
        kv_copy(s, lax.rem(s + i, S)).wait_recv()
    scale = 1.0 / math.sqrt(HD)
    column = lax.broadcasted_iota(jnp.int32, (L, W), 1)

    def head(h, unused):
        mine = (column >= h * HD) & (column < (h + 1) * HD)
        query = jnp.where(mine, q_ref[...].astype(F32), 0.0).astype(BF16)
        keys = kv[:, 0].reshape(S * L, W)
        values = kv[:, 1].reshape(S * L, W)
        scores = lax.dot_general(
            query, keys, (((1,), (1,)), ((), ())), preferred_element_type=F32
        ) * scale
        probs = jnp.exp(scores - jnp.max(scores, axis=1, keepdims=True))
        total = jnp.sum(probs, axis=1, keepdims=True)
        mixed = jnp.dot(probs.astype(BF16), values, preferred_element_type=F32) / total
        acc[...] = jnp.where(mine, mixed, acc[...])
        return unused

    acc[...] = jnp.zeros_like(acc)
    first = heads // 2
    if first:
        lax.fori_loop(0, first, head, jnp.int32(0))
    finish_send(order(S - 1))
    lax.fori_loop(first, heads, head, jnp.int32(0))
    attn_ref[...] = acc[...].astype(BF16)

    lane = lax.broadcasted_iota(jnp.int32, (T, S), 1)
    hit0 = ids_ref[:, 0:1] == lane
    hit1 = ids_ref[:, 1:2] == lane
    below = lax.broadcasted_iota(jnp.int32, (T, T), 1) < lax.broadcasted_iota(jnp.int32, (T, T), 0)
    before = jnp.dot(
        jnp.where(below, 1.0, 0.0).astype(BF16),
        jnp.where(hit0 | hit1, 1.0, 0.0).astype(BF16),
        preferred_element_type=F32,
    )
    base = before + (lane * capp).astype(F32)
    slot_lane = lax.broadcasted_iota(jnp.int32, (T, S * capp), 1).astype(F32)
    picks = [
        jnp.where(
            jnp.sum(jnp.where(hit, base, 0.0), axis=1, keepdims=True) == slot_lane, 1.0, 0.0
        ).astype(BF16)
        for hit in (hit0, hit1)
    ]
    for i in range(1, S):
        z_return(s, lax.rem(s + i, S)).wait_recv()
    everything = ret[...].reshape(S * capp, D)
    moe_ref[...] = (
        jnp.dot(picks[0], everything, preferred_element_type=F32) * gate_ref[:, 0:1]
        + jnp.dot(picks[1], everything, preferred_element_type=F32) * gate_ref[:, 1:2]
    ).astype(BF16)

    def drain(i, unused):
        to = lax.rem(s + i, S)
        z_copy(to, s).wait_send()
        kv_copy(to, s).wait_send()
        z_return(to, s).wait_send()
        return unused

    lax.fori_loop(1, S, drain, jnp.int32(0))

    def drain_chunk(i, unused):
        t_reduce(i).wait_send()
        for j in range(1, X):
            x_reduce(i, other_x(j), x).wait_send()
        return unused

    lax.fori_loop(0, S, drain_chunk, jnp.int32(0))


def local(
    attn_query, fresh_keys, fresh_values, stale_keys, stale_values, block_flags,
    moe_tokens, expert_ids, gate_weights, up_weight, up_bias, down_weight, down_bias,
):
    S, X = lax.axis_size("seq"), lax.axis_size("exp")
    assert lax.axis_size("tp") == 2 and up_weight.shape[0] == 1
    tokens, D = moe_tokens.shape
    length, width = attn_query.shape
    hidden = up_weight.shape[2]
    cap = 5 * tokens // (2 * S)
    capp = -(-cap // 16) * 16
    vmem = pl.BlockSpec(memory_space=pltpu.VMEM)
    smem = pl.BlockSpec(memory_space=pltpu.SMEM)
    hbm = pl.BlockSpec(memory_space=pl.ANY)
    dma = pltpu.SemaphoreType.DMA
    return pl.pallas_call(
        functools.partial(layer_kernel, (S, X, capp)),
        out_shape=(
            jax.ShapeDtypeStruct((length, width), BF16),
            jax.ShapeDtypeStruct((tokens, D), BF16),
        ),
        in_specs=[vmem] * 5 + [smem] + [vmem] * 4 + [hbm, vmem, hbm, vmem],
        out_specs=(vmem, vmem),
        scratch_shapes=[
            pltpu.VMEM((D, hidden), BF16),
            pltpu.VMEM((hidden, D), BF16),
            pltpu.VMEM((S, tokens), F32),
            pltpu.VMEM((S, capp, D), BF16),
            pltpu.VMEM((S, 2, X, capp, D), BF16),
            pltpu.VMEM((S, X, capp, D), BF16),
            pltpu.VMEM((S, X, capp, D), BF16),
            pltpu.VMEM((S, capp, D), BF16),
            pltpu.VMEM((S, capp, D), BF16),
            pltpu.VMEM((S, 2, length, width), BF16),
            pltpu.VMEM((length, width), F32),
            dma((2,)),
            dma((S,)), dma((S,)), dma((S, X)), dma((S, X)), dma((S, X)), dma((S, X)),
            dma((S,)), dma((S,)), dma((S, X)), dma((S, X)), dma((S,)), dma((S,)),
            dma((S,)), dma((S,)),
        ],
        compiler_params=pltpu.CompilerParams(
            collective_id=0, has_side_effects=True, vmem_limit_bytes=67043328
        ),
    )(
        attn_query, fresh_keys, fresh_values, stale_keys, stale_values, block_flags,
        moe_tokens, expert_ids, expert_ids.T, gate_weights,
        up_weight, up_bias, down_weight, down_bias,
    )


def solution(mesh):
    in_specs = (
        P(("groups", "seq"), ("exp", "tp")),
        P(("groups", "seq"), ("exp", "tp")),
        P(("groups", "seq"), ("exp", "tp")),
        P(("groups", "seq"), ("exp", "tp")),
        P(("groups", "seq"), ("exp", "tp")),
        P(("groups", "seq")),
        P(("groups", "seq", "exp", "tp"), None),
        P(("groups", "seq", "exp", "tp"), None),
        P(("groups", "seq", "exp", "tp"), None),
        P("seq", None, ("exp", "tp")),
        P("seq", ("exp", "tp")),
        P("seq", ("exp", "tp"), None),
        P("seq", None),
    )
    out_specs = (P(("groups", "seq"), ("exp", "tp")), P(("groups", "seq", "exp", "tp"), None))
    return jax.shard_map(local, mesh=mesh, in_specs=in_specs, out_specs=out_specs, check_vma=False)
```

```python
import functools
import math

import jax
import jax.numpy as jnp
from jax import lax
from jax.experimental import pallas as pl
from jax.experimental.pallas import tpu as pltpu
from jax.sharding import PartitionSpec as P

HD = 72
MESH = pl.DeviceIdType.MESH
F32 = jnp.float32
BF16 = jnp.bfloat16


def layer_kernel(
    sizes,
    q_ref, fresh_k, fresh_v, stale_k, stale_v, flags,
    tok_ref, ids_ref, gate_ref,
    up_hbm, upb_ref, down_hbm, downb_ref,
    attn_ref, moe_ref,
    up_v, down_v, place_v, disp, rows, tpin, xin, fin, ret, kv, keys_v, acc, turn,
    w_sem,
    z_send, z_recv, xf_send, xf_recv, tf_send, tf_recv,
    tr_send, tr_recv, xr_send, xr_recv, zr_send, zr_recv, kv_right, kv_left, kv_recv,
):
    S, X, capp = sizes
    s, x, c = lax.axis_index("seq"), lax.axis_index("exp"), lax.axis_index("tp")
    oc = 1 - c
    T, D = tok_ref.shape
    W, L = q_ref.shape
    heads = W // HD
    blk = L // flags.shape[0]

    up_copy = pltpu.make_async_copy(up_hbm.at[0], up_v, w_sem.at[0])
    down_copy = pltpu.make_async_copy(down_hbm.at[0], down_v, w_sem.at[1])
    up_copy.start()
    down_copy.start()

    def rdma(src, dst, ssem, rsem, where):
        return pltpu.make_async_remote_copy(
            src_ref=src, dst_ref=dst, send_sem=ssem, recv_sem=rsem,
            device_id=where, device_id_type=MESH,
        )

    def z_copy(e, slot):
        return rdma(disp.at[e], rows.at[slot, c, x], z_send.at[e], z_recv.at[slot], {"seq": e})

    def x_forward(src, to, origin):
        return rdma(
            rows.at[src, c, origin], rows.at[src, c, origin],
            xf_send.at[src, to], xf_recv.at[src, origin], {"exp": to},
        )

    def t_forward(src, origin, side):
        return rdma(
            rows.at[src, side, origin], rows.at[src, side, origin],
            tf_send.at[src, origin], tf_recv.at[src, origin], {"tp": oc},
        )

    def t_reduce(src):
        return rdma(rows.at[src, oc], tpin.at[src], tr_send.at[src], tr_recv.at[src], {"tp": oc})

    def x_reduce(src, to, origin):
        return rdma(
            rows.at[src, c, to], xin.at[src, origin],
            xr_send.at[src, to], xr_recv.at[src, origin], {"exp": to},
        )

    def z_return(src, slot):
        return rdma(fin.at[src], ret.at[slot], zr_send.at[src], zr_recv.at[slot], {"seq": src})

    def kv_copy(b, step):
        sems = kv_right if step > 0 else kv_left
        return rdma(kv.at[b], kv.at[b], sems.at[b], kv_recv.at[b], {"seq": s + step})

    def other_x(i):
        return lax.rem(x + i, X)

    def order(k):
        k = lax.rem(k + 1, S)
        half = (k + 1) // 2
        return lax.rem(s + half * (2 * lax.rem(k, 2) - 1) + S, S)

    barrier = pltpu.get_barrier_semaphore()
    for i in range(1, S):
        pl.semaphore_signal(barrier, inc=1, device_id={"seq": lax.rem(s + i, S)}, device_id_type=MESH)
    for i in range(1, X):
        pl.semaphore_signal(barrier, inc=1, device_id={"exp": other_x(i)}, device_id_type=MESH)
    pl.semaphore_signal(barrier, inc=1, device_id={"tp": oc}, device_id_type=MESH)

    expert = lax.broadcasted_iota(jnp.int32, (S, T), 0)
    named = (ids_ref[0:1, :] == expert) | (ids_ref[1:2, :] == expert)
    earlier = lax.broadcasted_iota(jnp.int32, (T, T), 0) < lax.broadcasted_iota(jnp.int32, (T, T), 1)
    place = jnp.dot(
        jnp.where(named, 1.0, 0.0).astype(BF16),
        jnp.where(earlier, 1.0, 0.0).astype(BF16),
        preferred_element_type=F32,
    )
    place_v[...] = jnp.where(named, place, -1.0)
    slot_rows = lax.broadcasted_iota(jnp.int32, (capp, T), 0).astype(F32)

    def slots_of(e):
        pick = jnp.where(place_v[pl.ds(e, 1), :] == slot_rows, 1.0, 0.0).astype(BF16)
        return jnp.dot(pick, tok_ref[...], preferred_element_type=F32).astype(BF16)

    def forward(src):
        for i in range(1, X):
            x_forward(src, other_x(i), x).start()
        t_forward(src, x, c).start()

    rows[s, c, x] = slots_of(s)
    pl.semaphore_wait(barrier, S - 1 + X - 1 + 1)
    forward(s)
    for k in range(S - 1):
        e = order(k)
        disp[e] = slots_of(e)
        z_copy(e, s).start()

    for b in range(flags.shape[0]):
        fresh = flags[b] == 1
        part = pl.ds(b * blk, blk)
        kv[s, 0, :, part] = jnp.where(fresh, fresh_k[:, part], stale_k[:, part])
        kv[s, 1, :, part] = jnp.where(fresh, fresh_v[:, part], stale_v[:, part])

    def relay(step):
        low, high = s - (step - 1), s + (step - 1)

        @pl.when(low >= 0)
        def _():
            @pl.when(low < s)
            def _():
                kv_copy(low, 1).wait_recv()

            @pl.when(s + 1 < S)
            def _():
                kv_copy(low, 1).start()

        @pl.when(high < S)
        def _():
            @pl.when(high > s)
            def _():
                kv_copy(high, -1).wait_recv()

            @pl.when(s - 1 >= 0)
            def _():
                kv_copy(high, -1).start()

    relay(jnp.int32(1))
    z_copy(order(0), order(0)).wait_recv()
    forward(order(0))

    up_copy.wait()
    down_copy.wait()

    def finish(src):
        total = rows[src, c, x].astype(F32) + downb_ref[...]
        for i in range(1, X):
            x_reduce(src, other_x(i), other_x(i)).wait_recv()
            total = total + xin[src, other_x(i)].astype(F32)
        done = total.astype(BF16)
        fin[src] = done

    def finish_send(src):
        finish(src)

        @pl.when(src != s)
        def _():
            z_return(src, s).start()

        @pl.when(src == s)
        def _():
            ret[s] = fin[s]

    def chunk(k, unused):
        src = order(k)
        for i in range(1, X):
            x_forward(src, other_x(i), other_x(i)).wait_recv()
            t_forward(src, other_x(i), c).start()

        @pl.when(k + 1 < S - 1)
        def _():
            nxt = order(k + 1)
            z_copy(nxt, nxt).wait_recv()
            forward(nxt)

        for i in range(X):
            t_forward(src, other_x(i), oc).wait_recv()
        for i in range(1, X):
            x_forward(src, other_x(i), x).wait_send()
        for i in range(X):
            t_forward(src, other_x(i), c).wait_send()

        block = rows[src].reshape(2 * X * capp, D)
        hidden = jnp.dot(block, up_v[...], preferred_element_type=F32) + upb_ref[...]
        hidden = jax.nn.gelu(hidden).astype(BF16)
        result = jnp.dot(hidden, down_v[...], preferred_element_type=F32).astype(BF16)
        rows[src] = result.reshape(2, X, capp, D)
        t_reduce(src).start()

        @pl.when(k >= 1)
        def _():
            finish_send(order(k - 1))
            relay(k + 1)

        t_reduce(src).wait_recv()
        for i in range(X):
            to = other_x(i)
            rows[src, c, to] = (rows[src, c, to].astype(F32) + tpin[src, to].astype(F32)).astype(BF16)
            if i > 0:
                x_reduce(src, to, x).start()
        return unused

    lax.fori_loop(0, S, chunk, jnp.int32(0))

    for i in range(S):
        keys_v[pl.ds(i * L, L), :] = kv[i, 0].T
    scale = 1.0 / math.sqrt(HD)
    channel = lax.broadcasted_iota(jnp.int32, (W, L), 0)

    def head(h, unused):
        mine = (channel >= h * HD) & (channel < (h + 1) * HD)
        query = jnp.where(mine, q_ref[...].astype(F32), 0.0).astype(BF16)
        scores = jnp.dot(keys_v[...], query, preferred_element_type=F32) * scale
        probs = jnp.exp(scores - jnp.max(scores, axis=0, keepdims=True))
        total = jnp.sum(probs, axis=0, keepdims=True)
        weights = probs.astype(BF16)
        mixed = jnp.zeros((W, L), F32)
        for i in range(S):
            mixed += jnp.dot(kv[i, 1], weights[i * L : (i + 1) * L], preferred_element_type=F32)
        acc[...] = jnp.where(mine, mixed / total, acc[...])
        return unused

    acc[...] = jnp.zeros_like(acc)
    lax.fori_loop(0, heads, head, jnp.int32(0))
    attn_ref[...] = acc[...].astype(BF16)
    finish_send(order(S - 1))

    base = jnp.where(named, place, 0.0) + (expert * capp).astype(F32)
    turn[...] = jnp.zeros_like(turn)
    for j in range(2):
        hit = ids_ref[j : j + 1, :] == expert
        turn[j : j + 1, :] = jnp.sum(jnp.where(hit, base, 0.0), axis=0, keepdims=True)
        turn[2 + j : 3 + j, :] = gate_ref[j : j + 1, :]
    turned = turn[...].T
    slot_lane = lax.broadcasted_iota(jnp.int32, (T, S * capp), 1).astype(F32)
    picks = [jnp.where(turned[:, j : j + 1] == slot_lane, 1.0, 0.0).astype(BF16) for j in range(2)]
    for i in range(1, S):
        z_return(s, lax.rem(s + i, S)).wait_recv()
    everything = ret[...].reshape(S * capp, D)
    moe_ref[...] = (
        jnp.dot(picks[0], everything, preferred_element_type=F32) * turned[:, 2:3]
        + jnp.dot(picks[1], everything, preferred_element_type=F32) * turned[:, 3:4]
    ).astype(BF16)

    def drain(i, unused):
        to = lax.rem(s + i, S)
        z_copy(to, s).wait_send()
        z_return(to, s).wait_send()
        return unused

    lax.fori_loop(1, S, drain, jnp.int32(0))

    def drain_chunk(i, unused):
        t_reduce(i).wait_send()
        for j in range(1, X):
            x_reduce(i, other_x(j), x).wait_send()

        @pl.when((i <= s) & (s + 1 < S))
        def _():
            kv_copy(i, 1).wait_send()

        @pl.when((i >= s) & (s - 1 >= 0))
        def _():
            kv_copy(i, -1).wait_send()

        return unused

    lax.fori_loop(0, S, drain_chunk, jnp.int32(0))


def local(
    attn_query, fresh_keys, fresh_values, stale_keys, stale_values, block_flags,
    moe_tokens, expert_ids, gate_weights, up_weight, up_bias, down_weight, down_bias,
):
    S, X = lax.axis_size("seq"), lax.axis_size("exp")
    assert lax.axis_size("tp") == 2 and up_weight.shape[0] == 1
    tokens, D = moe_tokens.shape
    length, width = attn_query.shape
    hidden = up_weight.shape[2]
    cap = 5 * tokens // (2 * S)
    capp = -(-cap // 16) * 16
    vmem = pl.BlockSpec(memory_space=pltpu.VMEM)
    smem = pl.BlockSpec(memory_space=pltpu.SMEM)
    hbm = pl.BlockSpec(memory_space=pl.ANY)
    dma = pltpu.SemaphoreType.DMA
    attn_out, moe_out = pl.pallas_call(
        functools.partial(layer_kernel, (S, X, capp)),
        out_shape=(
            jax.ShapeDtypeStruct((width, length), BF16),
            jax.ShapeDtypeStruct((tokens, D), BF16),
        ),
        in_specs=[vmem] * 5 + [smem] + [vmem] * 3 + [hbm, vmem, hbm, vmem],
        out_specs=(vmem, vmem),
        scratch_shapes=[
            pltpu.VMEM((D, hidden), BF16),
            pltpu.VMEM((hidden, D), BF16),
            pltpu.VMEM((S, tokens), F32),
            pltpu.VMEM((S, capp, D), BF16),
            pltpu.VMEM((S, 2, X, capp, D), BF16),
            pltpu.VMEM((S, X, capp, D), BF16),
            pltpu.VMEM((S, X, capp, D), BF16),
            pltpu.VMEM((S, capp, D), BF16),
            pltpu.VMEM((S, capp, D), BF16),
            pltpu.VMEM((S, 2, width, length), BF16),
            pltpu.VMEM((S * length, width), BF16),
            pltpu.VMEM((width, length), F32),
            pltpu.VMEM((128, tokens), F32),
            dma((2,)),
            dma((S,)), dma((S,)), dma((S, X)), dma((S, X)), dma((S, X)), dma((S, X)),
            dma((S,)), dma((S,)), dma((S, X)), dma((S, X)), dma((S,)), dma((S,)),
            dma((S,)), dma((S,)), dma((S,)),
        ],
        compiler_params=pltpu.CompilerParams(
            collective_id=0, has_side_effects=True, vmem_limit_bytes=67043328
        ),
    )(
        attn_query.T, fresh_keys.T, fresh_values.T, stale_keys.T, stale_values.T, block_flags,
        moe_tokens, expert_ids.T, gate_weights.T,
        up_weight, up_bias, down_weight, down_bias,
    )
    return attn_out.T, moe_out


def solution(mesh):
    in_specs = (
        P(("groups", "seq"), ("exp", "tp")),
        P(("groups", "seq"), ("exp", "tp")),
        P(("groups", "seq"), ("exp", "tp")),
        P(("groups", "seq"), ("exp", "tp")),
        P(("groups", "seq"), ("exp", "tp")),
        P(("groups", "seq")),
        P(("groups", "seq", "exp", "tp"), None),
        P(("groups", "seq", "exp", "tp"), None),
        P(("groups", "seq", "exp", "tp"), None),
        P("seq", None, ("exp", "tp")),
        P("seq", ("exp", "tp")),
        P("seq", ("exp", "tp"), None),
        P("seq", None),
    )
    out_specs = (P(("groups", "seq"), ("exp", "tp")), P(("groups", "seq", "exp", "tp"), None))
    return jax.shard_map(local, mesh=mesh, in_specs=in_specs, out_specs=out_specs, check_vma=False)
```

```python
import functools
import math

import jax
import jax.numpy as jnp
from jax import lax
from jax.experimental import pallas as pl
from jax.experimental.pallas import tpu as pltpu
from jax.sharding import PartitionSpec as P

HD = 72
MESH = pl.DeviceIdType.MESH
F32 = jnp.float32
BF16 = jnp.bfloat16


def layer_kernel(
    sizes,
    q_ref, fresh_k, fresh_v, stale_k, stale_v, flags,
    tok_ref, ids_ref, gate_ref,
    up_hbm, upb_ref, down_hbm, downb_ref,
    attn_ref, moe_ref,
    up_v, down_v, place_v, disp, rows, tpin, xin, fin, ret, kv, keys_v, acc, turn,
    w_sem,
    z_send, z_recv, xf_send, xf_recv, tf_send, tf_recv,
    tr_send, tr_recv, xr_send, xr_recv, zr_send, zr_recv, kv_right, kv_left, kv_recv,
):
    S, X, capp = sizes
    s, x, c = lax.axis_index("seq"), lax.axis_index("exp"), lax.axis_index("tp")
    oc = 1 - c
    T, D = tok_ref.shape
    W, L = q_ref.shape
    heads = W // HD
    blk = L // flags.shape[0]

    up_copy = pltpu.make_async_copy(up_hbm.at[0], up_v, w_sem.at[0])
    down_copy = pltpu.make_async_copy(down_hbm.at[0], down_v, w_sem.at[1])
    up_copy.start()
    down_copy.start()

    def rdma(src, dst, ssem, rsem, where):
        return pltpu.make_async_remote_copy(
            src_ref=src, dst_ref=dst, send_sem=ssem, recv_sem=rsem,
            device_id=where, device_id_type=MESH,
        )

    def z_copy(e, slot):
        return rdma(disp.at[e], rows.at[slot, c, x], z_send.at[e], z_recv.at[slot], {"seq": e})

    def x_forward(src, to, origin):
        return rdma(
            rows.at[src, c, origin], rows.at[src, c, origin],
            xf_send.at[src, to], xf_recv.at[src, origin], {"exp": to},
        )

    def t_forward(src, origin, side):
        return rdma(
            rows.at[src, side, origin], rows.at[src, side, origin],
            tf_send.at[src, origin], tf_recv.at[src, origin], {"tp": oc},
        )

    def t_reduce(src):
        return rdma(rows.at[src, oc], tpin.at[src], tr_send.at[src], tr_recv.at[src], {"tp": oc})

    def x_reduce(src, to, origin):
        return rdma(
            rows.at[src, c, to], xin.at[src, origin],
            xr_send.at[src, to], xr_recv.at[src, origin], {"exp": to},
        )

    def z_return(src, slot):
        return rdma(fin.at[src], ret.at[slot], zr_send.at[src], zr_recv.at[slot], {"seq": src})

    def kv_copy(b, step):
        sems = kv_right if step > 0 else kv_left
        return rdma(kv.at[b], kv.at[b], sems.at[b], kv_recv.at[b], {"seq": s + step})

    def other_x(i):
        return lax.rem(x + i, X)

    def order(k):
        side = jnp.minimum(s, S - 1 - s)
        near = k // 2 + 1
        near = jnp.where(lax.rem(k, 2) == 0, near, -near)
        far = k - side + 1
        far = jnp.where(2 * s < S, far, -far)
        step = jnp.where(k < 2 * side, near, far)
        return s + jnp.where(k == S - 1, 0, step)

    barrier = pltpu.get_barrier_semaphore()
    for i in range(1, S):
        pl.semaphore_signal(barrier, inc=1, device_id={"seq": lax.rem(s + i, S)}, device_id_type=MESH)
    for i in range(1, X):
        pl.semaphore_signal(barrier, inc=1, device_id={"exp": other_x(i)}, device_id_type=MESH)
    pl.semaphore_signal(barrier, inc=1, device_id={"tp": oc}, device_id_type=MESH)

    expert = lax.broadcasted_iota(jnp.int32, (S, T), 0)
    named = (ids_ref[0:1, :] == expert) | (ids_ref[1:2, :] == expert)
    earlier = lax.broadcasted_iota(jnp.int32, (T, T), 0) < lax.broadcasted_iota(jnp.int32, (T, T), 1)
    place = jnp.dot(
        jnp.where(named, 1.0, 0.0).astype(BF16),
        jnp.where(earlier, 1.0, 0.0).astype(BF16),
        preferred_element_type=F32,
    )
    place_v[...] = jnp.where(named, place, -1.0)
    slot_rows = lax.broadcasted_iota(jnp.int32, (capp, T), 0).astype(F32)

    def slots_of(e):
        pick = jnp.where(place_v[pl.ds(e, 1), :] == slot_rows, 1.0, 0.0).astype(BF16)
        return jnp.dot(pick, tok_ref[...], preferred_element_type=F32).astype(BF16)

    def forward(src):
        for i in range(1, X):
            x_forward(src, other_x(i), x).start()
        t_forward(src, x, c).start()

    rows[s, c, x] = slots_of(s)
    pl.semaphore_wait(barrier, S - 1 + X - 1 + 1)
    forward(s)
    def dispatch(k):
        e = order(jnp.int32(k))
        disp[e] = slots_of(e)
        z_copy(e, s).start()

    for k in range(min(2, S - 1)):
        dispatch(k)
    for b in range(flags.shape[0]):
        fresh = flags[b] == 1
        part = pl.ds(b * blk, blk)
        kv[s, 0, :, part] = jnp.where(fresh, fresh_k[:, part], stale_k[:, part])
        kv[s, 1, :, part] = jnp.where(fresh, fresh_v[:, part], stale_v[:, part])

    def relay(step):
        low, high = s - (step - 1), s + (step - 1)

        @pl.when(low >= 0)
        def _():
            @pl.when(low < s)
            def _():
                kv_copy(low, 1).wait_recv()

            @pl.when(s + 1 < S)
            def _():
                kv_copy(low, 1).start()

        @pl.when(high < S)
        def _():
            @pl.when(high > s)
            def _():
                kv_copy(high, -1).wait_recv()

            @pl.when(s - 1 >= 0)
            def _():
                kv_copy(high, -1).start()

    relay(1)
    for k in range(2, S - 1):
        dispatch(k)
    nearest = order(jnp.int32(0))
    z_copy(nearest, nearest).wait_recv()
    forward(nearest)

    up_copy.wait()
    down_copy.wait()

    def finish(src):
        total = rows[src, c, x].astype(F32) + downb_ref[...]
        for i in range(1, X):
            x_reduce(src, other_x(i), other_x(i)).wait_recv()
            total = total + xin[src, other_x(i)].astype(F32)
        done = total.astype(BF16)
        fin[src] = done

    def finish_send(src):
        finish(src)

        @pl.when(src != s)
        def _():
            z_return(src, s).start()

        @pl.when(src == s)
        def _():
            ret[s] = fin[s]

    def chunk(k, unused):
        src = order(k)
        for i in range(1, X):
            x_forward(src, other_x(i), other_x(i)).wait_recv()
            t_forward(src, other_x(i), c).start()

        @pl.when(k + 1 < S - 1)
        def _():
            nxt = order(k + 1)
            z_copy(nxt, nxt).wait_recv()
            forward(nxt)

        for i in range(X):
            t_forward(src, other_x(i), oc).wait_recv()
        for i in range(1, X):
            x_forward(src, other_x(i), x).wait_send()
        for i in range(X):
            t_forward(src, other_x(i), c).wait_send()

        block = rows[src].reshape(2 * X * capp, D)
        hidden = jnp.dot(block, up_v[...], preferred_element_type=F32) + upb_ref[...]
        hidden = jax.nn.gelu(hidden).astype(BF16)
        result = jnp.dot(hidden, down_v[...], preferred_element_type=F32).astype(BF16)
        rows[src] = result.reshape(2, X, capp, D)
        t_reduce(src).start()

        @pl.when(k >= 1)
        def _():
            finish_send(order(k - 1))

        @pl.when(k == 0)
        def _():
            relay(2)

        @pl.when((k >= 2) & (k < S - 1))
        def _():
            relay(k + 1)

        t_reduce(src).wait_recv()
        for i in range(X):
            to = other_x(i)
            rows[src, c, to] = (rows[src, c, to].astype(F32) + tpin[src, to].astype(F32)).astype(BF16)
            if i > 0:
                x_reduce(src, to, x).start()
        return unused

    lax.fori_loop(0, S, chunk, jnp.int32(0))

    relay(S)

    for i in range(S):
        keys_v[pl.ds(i * L, L), :] = kv[i, 0].T
    scale = 1.0 / math.sqrt(HD)
    channel = lax.broadcasted_iota(jnp.int32, (W, L), 0)

    def head(h, unused):
        mine = (channel >= h * HD) & (channel < (h + 1) * HD)
        query = jnp.where(mine, q_ref[...].astype(F32), 0.0).astype(BF16)
        scores = jnp.dot(keys_v[...], query, preferred_element_type=F32) * scale
        probs = jnp.exp(scores - jnp.max(scores, axis=0, keepdims=True))
        total = jnp.sum(probs, axis=0, keepdims=True)
        weights = probs.astype(BF16)
        mixed = jnp.zeros((W, L), F32)
        for i in range(S):
            mixed += jnp.dot(kv[i, 1], weights[i * L : (i + 1) * L], preferred_element_type=F32)
        acc[...] = jnp.where(mine, mixed / total, acc[...])
        return unused

    acc[...] = jnp.zeros_like(acc)
    lax.fori_loop(0, heads, head, jnp.int32(0))
    attn_ref[...] = acc[...].astype(BF16)
    finish_send(s)

    base = jnp.where(named, place, 0.0) + (expert * capp).astype(F32)
    turn[...] = jnp.zeros_like(turn)
    for j in range(2):
        hit = ids_ref[j : j + 1, :] == expert
        turn[j : j + 1, :] = jnp.sum(jnp.where(hit, base, 0.0), axis=0, keepdims=True)
        turn[2 + j : 3 + j, :] = gate_ref[j : j + 1, :]
    turned = turn[...].T
    slot_lane = lax.broadcasted_iota(jnp.int32, (T, S * capp), 1).astype(F32)
    picks = [jnp.where(turned[:, j : j + 1] == slot_lane, 1.0, 0.0).astype(BF16) for j in range(2)]
    for i in range(1, S):
        z_return(s, lax.rem(s + i, S)).wait_recv()
    everything = ret[...].reshape(S * capp, D)
    moe_ref[...] = (
        jnp.dot(picks[0], everything, preferred_element_type=F32) * turned[:, 2:3]
        + jnp.dot(picks[1], everything, preferred_element_type=F32) * turned[:, 3:4]
    ).astype(BF16)

    def drain(i, unused):
        to = lax.rem(s + i, S)
        z_copy(to, s).wait_send()
        z_return(to, s).wait_send()
        return unused

    lax.fori_loop(1, S, drain, jnp.int32(0))

    def drain_chunk(i, unused):
        t_reduce(i).wait_send()
        for j in range(1, X):
            x_reduce(i, other_x(j), x).wait_send()

        @pl.when((i <= s) & (s + 1 < S))
        def _():
            kv_copy(i, 1).wait_send()

        @pl.when((i >= s) & (s - 1 >= 0))
        def _():
            kv_copy(i, -1).wait_send()

        return unused

    lax.fori_loop(0, S, drain_chunk, jnp.int32(0))


def local(
    attn_query, fresh_keys, fresh_values, stale_keys, stale_values, block_flags,
    moe_tokens, expert_ids, gate_weights, up_weight, up_bias, down_weight, down_bias,
):
    S, X = lax.axis_size("seq"), lax.axis_size("exp")
    assert lax.axis_size("tp") == 2 and up_weight.shape[0] == 1
    tokens, D = moe_tokens.shape
    length, width = attn_query.shape
    hidden = up_weight.shape[2]
    cap = 5 * tokens // (2 * S)
    capp = -(-cap // 16) * 16
    vmem = pl.BlockSpec(memory_space=pltpu.VMEM)
    smem = pl.BlockSpec(memory_space=pltpu.SMEM)
    hbm = pl.BlockSpec(memory_space=pl.ANY)
    dma = pltpu.SemaphoreType.DMA
    attn_out, moe_out = pl.pallas_call(
        functools.partial(layer_kernel, (S, X, capp)),
        out_shape=(
            jax.ShapeDtypeStruct((width, length), BF16),
            jax.ShapeDtypeStruct((tokens, D), BF16),
        ),
        in_specs=[vmem] * 5 + [smem] + [vmem] * 3 + [hbm, vmem, hbm, vmem],
        out_specs=(vmem, vmem),
        scratch_shapes=[
            pltpu.VMEM((D, hidden), BF16),
            pltpu.VMEM((hidden, D), BF16),
            pltpu.VMEM((S, tokens), F32),
            pltpu.VMEM((S, capp, D), BF16),
            pltpu.VMEM((S, 2, X, capp, D), BF16),
            pltpu.VMEM((S, X, capp, D), BF16),
            pltpu.VMEM((S, X, capp, D), BF16),
            pltpu.VMEM((S, capp, D), BF16),
            pltpu.VMEM((S, capp, D), BF16),
            pltpu.VMEM((S, 2, width, length), BF16),
            pltpu.VMEM((S * length, width), BF16),
            pltpu.VMEM((width, length), F32),
            pltpu.VMEM((128, tokens), F32),
            dma((2,)),
            dma((S,)), dma((S,)), dma((S, X)), dma((S, X)), dma((S, X)), dma((S, X)),
            dma((S,)), dma((S,)), dma((S, X)), dma((S, X)), dma((S,)), dma((S,)),
            dma((S,)), dma((S,)), dma((S,)),
        ],
        compiler_params=pltpu.CompilerParams(
            collective_id=0, has_side_effects=True, vmem_limit_bytes=67043328
        ),
    )(
        attn_query.T, fresh_keys.T, fresh_values.T, stale_keys.T, stale_values.T, block_flags,
        moe_tokens, expert_ids.T, gate_weights.T,
        up_weight, up_bias, down_weight, down_bias,
    )
    return attn_out.T, moe_out


def solution(mesh):
    in_specs = (
        P(("groups", "seq"), ("exp", "tp")),
        P(("groups", "seq"), ("exp", "tp")),
        P(("groups", "seq"), ("exp", "tp")),
        P(("groups", "seq"), ("exp", "tp")),
        P(("groups", "seq"), ("exp", "tp")),
        P(("groups", "seq")),
        P(("groups", "seq", "exp", "tp"), None),
        P(("groups", "seq", "exp", "tp"), None),
        P(("groups", "seq", "exp", "tp"), None),
        P("seq", None, ("exp", "tp")),
        P("seq", ("exp", "tp")),
        P("seq", ("exp", "tp"), None),
        P("seq", None),
    )
    out_specs = (P(("groups", "seq"), ("exp", "tp")), P(("groups", "seq", "exp", "tp"), None))
    return jax.shard_map(local, mesh=mesh, in_specs=in_specs, out_specs=out_specs, check_vma=False)
```

```python
import functools
import math

import jax
import jax.numpy as jnp
from jax import lax
from jax.experimental import pallas as pl
from jax.experimental.pallas import tpu as pltpu
from jax.sharding import PartitionSpec as P

HD = 72
MESH = pl.DeviceIdType.MESH
F32 = jnp.float32
BF16 = jnp.bfloat16


def layer_kernel(
    sizes,
    q_ref, fresh_k, fresh_v, stale_k, stale_v, flags,
    tok_ref, ids_ref, gate_ref,
    up_hbm, upb_ref, down_hbm, downb_ref,
    attn_ref, moe_ref,
    up_v, down_v, place_v, disp, rows, tpin, xin, fin, ret, kv, keys_v, acc, turn,
    w_sem,
    z_send, z_recv, xf_send, xf_recv, tf_send, tf_recv,
    tr_send, tr_recv, xr_send, xr_recv, zr_send, zr_recv, kv_right, kv_left, kv_recv,
):
    S, X, capp = sizes
    s, x, c = lax.axis_index("seq"), lax.axis_index("exp"), lax.axis_index("tp")
    oc = 1 - c
    T, D = tok_ref.shape
    W, L = q_ref.shape
    heads = W // HD
    blk = L // flags.shape[0]

    up_copy = pltpu.make_async_copy(up_hbm.at[0], up_v, w_sem.at[0])
    down_copy = pltpu.make_async_copy(down_hbm.at[0], down_v, w_sem.at[1])
    up_copy.start()
    down_copy.start()

    def rdma(src, dst, ssem, rsem, where):
        return pltpu.make_async_remote_copy(
            src_ref=src, dst_ref=dst, send_sem=ssem, recv_sem=rsem,
            device_id=where, device_id_type=MESH,
        )

    def z_copy(e, slot):
        return rdma(disp.at[e], rows.at[slot, c, x], z_send.at[e], z_recv.at[slot], {"seq": e})

    def x_forward(src, to, origin):
        return rdma(
            rows.at[src, c, origin], rows.at[src, c, origin],
            xf_send.at[src, to], xf_recv.at[src, origin], {"exp": to},
        )

    def t_forward(src, origin, side):
        return rdma(
            rows.at[src, side, origin], rows.at[src, side, origin],
            tf_send.at[src, origin], tf_recv.at[src, origin], {"tp": oc},
        )

    def t_reduce(src):
        return rdma(rows.at[src, oc], tpin.at[src], tr_send.at[src], tr_recv.at[src], {"tp": oc})

    def x_reduce(src, to, origin):
        return rdma(
            rows.at[src, c, to], xin.at[src, origin],
            xr_send.at[src, to], xr_recv.at[src, origin], {"exp": to},
        )

    def z_return(src, slot):
        return rdma(fin.at[src], ret.at[slot], zr_send.at[src], zr_recv.at[slot], {"seq": src})

    def kv_copy(b, step):
        sems = kv_right if step > 0 else kv_left
        return rdma(kv.at[b], kv.at[b], sems.at[b], kv_recv.at[b], {"seq": s + step})

    def other_x(i):
        return lax.rem(x + i, X)

    side = jnp.minimum(s, S - 1 - s)
    own_turn = jnp.maximum(1, 2 * side)

    def remote(j):
        near = j // 2 + 1
        near = jnp.where(lax.rem(j, 2) == 0, near, -near)
        far = j - side + 1
        far = jnp.where(2 * s < S, far, -far)
        return s + jnp.where(j < 2 * side, near, far)

    def order(k):
        return jnp.where(k == own_turn, s, remote(jnp.where(k > own_turn, k - 1, k)))

    barrier = pltpu.get_barrier_semaphore()
    for i in range(1, S):
        pl.semaphore_signal(barrier, inc=1, device_id={"seq": lax.rem(s + i, S)}, device_id_type=MESH)
    for i in range(1, X):
        pl.semaphore_signal(barrier, inc=1, device_id={"exp": other_x(i)}, device_id_type=MESH)
    pl.semaphore_signal(barrier, inc=1, device_id={"tp": oc}, device_id_type=MESH)

    expert = lax.broadcasted_iota(jnp.int32, (S, T), 0)
    named = (ids_ref[0:1, :] == expert) | (ids_ref[1:2, :] == expert)
    earlier = lax.broadcasted_iota(jnp.int32, (T, T), 0) < lax.broadcasted_iota(jnp.int32, (T, T), 1)
    place = jnp.dot(
        jnp.where(named, 1.0, 0.0).astype(BF16),
        jnp.where(earlier, 1.0, 0.0).astype(BF16),
        preferred_element_type=F32,
    )
    place_v[...] = jnp.where(named, place, -1.0)
    slot_rows = lax.broadcasted_iota(jnp.int32, (capp, T), 0).astype(F32)

    def slots_of(e):
        pick = jnp.where(place_v[pl.ds(e, 1), :] == slot_rows, 1.0, 0.0).astype(BF16)
        return jnp.dot(pick, tok_ref[...], preferred_element_type=F32).astype(BF16)

    def forward(src):
        for i in range(1, X):
            x_forward(src, other_x(i), x).start()
        t_forward(src, x, c).start()

    rows[s, c, x] = slots_of(s)
    pl.semaphore_wait(barrier, S - 1 + X - 1 + 1)
    forward(s)
    for j in range(S - 1):
        e = remote(jnp.int32(j))
        disp[e] = slots_of(e)
        z_copy(e, s).start()

    for b in range(flags.shape[0]):
        fresh = flags[b] == 1
        part = pl.ds(b * blk, blk)
        kv[s, 0, :, part] = jnp.where(fresh, fresh_k[:, part], stale_k[:, part])
        kv[s, 1, :, part] = jnp.where(fresh, fresh_v[:, part], stale_v[:, part])

    def relay(step):
        low, high = s - (step - 1), s + (step - 1)

        @pl.when(low >= 0)
        def _():
            @pl.when(low < s)
            def _():
                kv_copy(low, 1).wait_recv()

            @pl.when(s + 1 < S)
            def _():
                kv_copy(low, 1).start()

        @pl.when(high < S)
        def _():
            @pl.when(high > s)
            def _():
                kv_copy(high, -1).wait_recv()

            @pl.when(s - 1 >= 0)
            def _():
                kv_copy(high, -1).start()

    relay(1)
    nearest = order(jnp.int32(0))
    z_copy(nearest, nearest).wait_recv()
    forward(nearest)

    up_copy.wait()
    down_copy.wait()

    def finish(src):
        total = rows[src, c, x].astype(F32) + downb_ref[...]
        for i in range(1, X):
            x_reduce(src, other_x(i), other_x(i)).wait_recv()
            total = total + xin[src, other_x(i)].astype(F32)
        done = total.astype(BF16)
        fin[src] = done

    def finish_send(src):
        finish(src)

        @pl.when(src != s)
        def _():
            z_return(src, s).start()

        @pl.when(src == s)
        def _():
            ret[s] = fin[s]

    def chunk(k, unused):
        src = order(k)
        for i in range(1, X):
            x_forward(src, other_x(i), other_x(i)).wait_recv()
            t_forward(src, other_x(i), c).start()

        nxt = order(k + 1)
        late = (k == own_turn) & (k == 1)

        @pl.when((k + 1 < S) & (nxt != s) & jnp.logical_not(late))
        def _():
            z_copy(nxt, nxt).wait_recv()
            forward(nxt)

        for i in range(X):
            t_forward(src, other_x(i), oc).wait_recv()
        for i in range(1, X):
            x_forward(src, other_x(i), x).wait_send()
        for i in range(X):
            t_forward(src, other_x(i), c).wait_send()

        block = rows[src].reshape(2 * X * capp, D)
        hidden = jnp.dot(block, up_v[...], preferred_element_type=F32) + upb_ref[...]
        hidden = jax.nn.gelu(hidden).astype(BF16)
        result = jnp.dot(hidden, down_v[...], preferred_element_type=F32).astype(BF16)
        rows[src] = result.reshape(2, X, capp, D)
        t_reduce(src).start()

        @pl.when(k >= 1)
        def _():
            finish_send(order(k - 1))

        @pl.when((k + 1 < S) & late)
        def _():
            z_copy(nxt, nxt).wait_recv()
            forward(nxt)

        @pl.when((k >= 1) & (k < S - 1))
        def _():
            relay(k + 1)

        t_reduce(src).wait_recv()
        for i in range(X):
            to = other_x(i)
            rows[src, c, to] = (rows[src, c, to].astype(F32) + tpin[src, to].astype(F32)).astype(BF16)
            if i > 0:
                x_reduce(src, to, x).start()
        return unused

    lax.fori_loop(0, S, chunk, jnp.int32(0))

    relay(S)

    for i in range(S):
        keys_v[pl.ds(i * L, L), :] = kv[i, 0].T
    scale = 1.0 / math.sqrt(HD)
    channel = lax.broadcasted_iota(jnp.int32, (W, L), 0)

    def head(h, unused):
        mine = (channel >= h * HD) & (channel < (h + 1) * HD)
        query = jnp.where(mine, q_ref[...].astype(F32), 0.0).astype(BF16)
        scores = jnp.dot(keys_v[...], query, preferred_element_type=F32) * scale
        probs = jnp.exp(scores - jnp.max(scores, axis=0, keepdims=True))
        total = jnp.sum(probs, axis=0, keepdims=True)
        weights = probs.astype(BF16)
        mixed = jnp.zeros((W, L), F32)
        for i in range(S):
            mixed += jnp.dot(kv[i, 1], weights[i * L : (i + 1) * L], preferred_element_type=F32)
        acc[...] = jnp.where(mine, mixed / total, acc[...])
        return unused

    acc[...] = jnp.zeros_like(acc)
    lax.fori_loop(0, heads, head, jnp.int32(0))
    attn_ref[...] = acc[...].astype(BF16)
    finish_send(order(S - 1))

    base = jnp.where(named, place, 0.0) + (expert * capp).astype(F32)
    turn[...] = jnp.zeros_like(turn)
    for j in range(2):
        hit = ids_ref[j : j + 1, :] == expert
        turn[j : j + 1, :] = jnp.sum(jnp.where(hit, base, 0.0), axis=0, keepdims=True)
        turn[2 + j : 3 + j, :] = gate_ref[j : j + 1, :]
    turned = turn[...].T
    slot_lane = lax.broadcasted_iota(jnp.int32, (T, S * capp), 1).astype(F32)
    picks = [jnp.where(turned[:, j : j + 1] == slot_lane, 1.0, 0.0).astype(BF16) for j in range(2)]
    for i in range(1, S):
        z_return(s, lax.rem(s + i, S)).wait_recv()
    everything = ret[...].reshape(S * capp, D)
    moe_ref[...] = (
        jnp.dot(picks[0], everything, preferred_element_type=F32) * turned[:, 2:3]
        + jnp.dot(picks[1], everything, preferred_element_type=F32) * turned[:, 3:4]
    ).astype(BF16)

    def drain(i, unused):
        to = lax.rem(s + i, S)
        z_copy(to, s).wait_send()
        z_return(to, s).wait_send()
        return unused

    lax.fori_loop(1, S, drain, jnp.int32(0))

    def drain_chunk(i, unused):
        t_reduce(i).wait_send()
        for j in range(1, X):
            x_reduce(i, other_x(j), x).wait_send()

        @pl.when((i <= s) & (s + 1 < S))
        def _():
            kv_copy(i, 1).wait_send()

        @pl.when((i >= s) & (s - 1 >= 0))
        def _():
            kv_copy(i, -1).wait_send()

        return unused

    lax.fori_loop(0, S, drain_chunk, jnp.int32(0))


def local(
    attn_query, fresh_keys, fresh_values, stale_keys, stale_values, block_flags,
    moe_tokens, expert_ids, gate_weights, up_weight, up_bias, down_weight, down_bias,
):
    S, X = lax.axis_size("seq"), lax.axis_size("exp")
    assert lax.axis_size("tp") == 2 and up_weight.shape[0] == 1
    tokens, D = moe_tokens.shape
    length, width = attn_query.shape
    hidden = up_weight.shape[2]
    cap = 5 * tokens // (2 * S)
    capp = -(-cap // 16) * 16
    vmem = pl.BlockSpec(memory_space=pltpu.VMEM)
    smem = pl.BlockSpec(memory_space=pltpu.SMEM)
    hbm = pl.BlockSpec(memory_space=pl.ANY)
    dma = pltpu.SemaphoreType.DMA
    attn_out, moe_out = pl.pallas_call(
        functools.partial(layer_kernel, (S, X, capp)),
        out_shape=(
            jax.ShapeDtypeStruct((width, length), BF16),
            jax.ShapeDtypeStruct((tokens, D), BF16),
        ),
        in_specs=[vmem] * 5 + [smem] + [vmem] * 3 + [hbm, vmem, hbm, vmem],
        out_specs=(vmem, vmem),
        scratch_shapes=[
            pltpu.VMEM((D, hidden), BF16),
            pltpu.VMEM((hidden, D), BF16),
            pltpu.VMEM((S, tokens), F32),
            pltpu.VMEM((S, capp, D), BF16),
            pltpu.VMEM((S, 2, X, capp, D), BF16),
            pltpu.VMEM((S, X, capp, D), BF16),
            pltpu.VMEM((S, X, capp, D), BF16),
            pltpu.VMEM((S, capp, D), BF16),
            pltpu.VMEM((S, capp, D), BF16),
            pltpu.VMEM((S, 2, width, length), BF16),
            pltpu.VMEM((S * length, width), BF16),
            pltpu.VMEM((width, length), F32),
            pltpu.VMEM((128, tokens), F32),
            dma((2,)),
            dma((S,)), dma((S,)), dma((S, X)), dma((S, X)), dma((S, X)), dma((S, X)),
            dma((S,)), dma((S,)), dma((S, X)), dma((S, X)), dma((S,)), dma((S,)),
            dma((S,)), dma((S,)), dma((S,)),
        ],
        compiler_params=pltpu.CompilerParams(
            collective_id=0, has_side_effects=True, vmem_limit_bytes=67043328
        ),
    )(
        attn_query.T, fresh_keys.T, fresh_values.T, stale_keys.T, stale_values.T, block_flags,
        moe_tokens, expert_ids.T, gate_weights.T,
        up_weight, up_bias, down_weight, down_bias,
    )
    return attn_out.T, moe_out


def solution(mesh):
    in_specs = (
        P(("groups", "seq"), ("exp", "tp")),
        P(("groups", "seq"), ("exp", "tp")),
        P(("groups", "seq"), ("exp", "tp")),
        P(("groups", "seq"), ("exp", "tp")),
        P(("groups", "seq"), ("exp", "tp")),
        P(("groups", "seq")),
        P(("groups", "seq", "exp", "tp"), None),
        P(("groups", "seq", "exp", "tp"), None),
        P(("groups", "seq", "exp", "tp"), None),
        P("seq", None, ("exp", "tp")),
        P("seq", ("exp", "tp")),
        P("seq", ("exp", "tp"), None),
        P("seq", None),
    )
    out_specs = (P(("groups", "seq"), ("exp", "tp")), P(("groups", "seq", "exp", "tp"), None))
    return jax.shard_map(local, mesh=mesh, in_specs=in_specs, out_specs=out_specs, check_vma=False)
```

```python
import functools
import math

import jax
import jax.numpy as jnp
from jax import lax
from jax.experimental import pallas as pl
from jax.experimental.pallas import tpu as pltpu
from jax.sharding import PartitionSpec as P

HD = 72
MESH = pl.DeviceIdType.MESH
F32 = jnp.float32
BF16 = jnp.bfloat16


def layer_kernel(
    sizes,
    q_ref, fresh_k, fresh_v, stale_k, stale_v, flags,
    tok_ref, ids_ref, gate_ref,
    up_hbm, upb_ref, down_hbm, downb_ref,
    attn_ref, moe_ref,
    up_v, down_v, place_v, disp, rows, tpin, xin, fin, ret, kv, keys_v, acc, turn,
    w_sem,
    z_send, z_recv, xf_send, xf_recv, tf_send, tf_recv,
    tr_send, tr_recv, xr_send, xr_recv, zr_send, zr_recv, kv_right, kv_left, kv_recv,
):
    S, X, capp = sizes
    s, x, c = lax.axis_index("seq"), lax.axis_index("exp"), lax.axis_index("tp")
    oc = 1 - c
    T, D = tok_ref.shape
    W, L = q_ref.shape
    heads = W // HD
    blk = L // flags.shape[0]

    up_copy = pltpu.make_async_copy(up_hbm.at[0], up_v, w_sem.at[0])
    down_copy = pltpu.make_async_copy(down_hbm.at[0], down_v, w_sem.at[1])
    up_copy.start()
    down_copy.start()

    def rdma(src, dst, ssem, rsem, where):
        return pltpu.make_async_remote_copy(
            src_ref=src, dst_ref=dst, send_sem=ssem, recv_sem=rsem,
            device_id=where, device_id_type=MESH,
        )

    def z_copy(e, slot):
        return rdma(disp.at[e], rows.at[slot, c, x], z_send.at[e], z_recv.at[slot], {"seq": e})

    def x_forward(src, to, origin):
        return rdma(
            rows.at[src, c, origin], rows.at[src, c, origin],
            xf_send.at[src, to], xf_recv.at[src, origin], {"exp": to},
        )

    def t_forward(src, origin, side):
        return rdma(
            rows.at[src, side, origin], rows.at[src, side, origin],
            tf_send.at[src, origin], tf_recv.at[src, origin], {"tp": oc},
        )

    def t_reduce(src):
        return rdma(rows.at[src, oc], tpin.at[src], tr_send.at[src], tr_recv.at[src], {"tp": oc})

    def x_reduce(src, to, origin):
        return rdma(
            rows.at[src, c, to], xin.at[src, origin],
            xr_send.at[src, to], xr_recv.at[src, origin], {"exp": to},
        )

    def z_return(src, slot):
        return rdma(fin.at[src], ret.at[slot], zr_send.at[src], zr_recv.at[slot], {"seq": src})

    def kv_copy(b, step):
        sems = kv_right if step > 0 else kv_left
        return rdma(kv.at[b], kv.at[b], sems.at[b], kv_recv.at[b], {"seq": s + step})

    def other_x(i):
        return lax.rem(x + i, X)

    side = jnp.minimum(s, S - 1 - s)
    own_turn = jnp.maximum(1, 2 * side)

    def remote(j):
        near = j // 2 + 1
        near = jnp.where(lax.rem(j, 2) == 0, near, -near)
        far = j - side + 1
        far = jnp.where(2 * s < S, far, -far)
        return s + jnp.where(j < 2 * side, near, far)

    def order(k):
        return jnp.where(k == own_turn, s, remote(jnp.where(k > own_turn, k - 1, k)))

    barrier = pltpu.get_barrier_semaphore()
    for i in range(1, S):
        pl.semaphore_signal(barrier, inc=1, device_id={"seq": lax.rem(s + i, S)}, device_id_type=MESH)
    for i in range(1, X):
        pl.semaphore_signal(barrier, inc=1, device_id={"exp": other_x(i)}, device_id_type=MESH)
    pl.semaphore_signal(barrier, inc=1, device_id={"tp": oc}, device_id_type=MESH)

    expert = lax.broadcasted_iota(jnp.int32, (S, T), 0)
    named = (ids_ref[0:1, :] == expert) | (ids_ref[1:2, :] == expert)
    earlier = lax.broadcasted_iota(jnp.int32, (T, T), 0) < lax.broadcasted_iota(jnp.int32, (T, T), 1)
    place = jnp.dot(
        jnp.where(named, 1.0, 0.0).astype(BF16),
        jnp.where(earlier, 1.0, 0.0).astype(BF16),
        preferred_element_type=F32,
    )
    place_v[...] = jnp.where(named, place, -1.0)
    slot_rows = lax.broadcasted_iota(jnp.int32, (capp, T), 0).astype(F32)

    def slots_of(e):
        pick = jnp.where(place_v[pl.ds(e, 1), :] == slot_rows, 1.0, 0.0).astype(BF16)
        return jnp.dot(pick, tok_ref[...], preferred_element_type=F32).astype(BF16)

    def forward(src):
        for i in range(1, X):
            x_forward(src, other_x(i), x).start()
        t_forward(src, x, c).start()

    rows[s, c, x] = slots_of(s)
    pl.semaphore_wait(barrier, S - 1 + X - 1 + 1)
    forward(s)
    def dispatch(j):
        e = remote(jnp.int32(j))
        disp[e] = slots_of(e)
        z_copy(e, s).start()

    for j in range(min(2, S - 1)):
        dispatch(j)
    for b in range(flags.shape[0]):
        fresh = flags[b] == 1
        part = pl.ds(b * blk, blk)
        kv[s, 0, :, part] = jnp.where(fresh, fresh_k[:, part], stale_k[:, part])
        kv[s, 1, :, part] = jnp.where(fresh, fresh_v[:, part], stale_v[:, part])

    def relay(step):
        low, high = s - (step - 1), s + (step - 1)

        @pl.when(low >= 0)
        def _():
            @pl.when(low < s)
            def _():
                kv_copy(low, 1).wait_recv()

            @pl.when(s + 1 < S)
            def _():
                kv_copy(low, 1).start()

        @pl.when(high < S)
        def _():
            @pl.when(high > s)
            def _():
                kv_copy(high, -1).wait_recv()

            @pl.when(s - 1 >= 0)
            def _():
                kv_copy(high, -1).start()

    relay(1)
    for j in range(2, S - 1):
        dispatch(j)
    nearest = order(jnp.int32(0))
    z_copy(nearest, nearest).wait_recv()
    forward(nearest)

    up_copy.wait()
    down_copy.wait()

    def finish(src):
        total = rows[src, c, x].astype(F32) + downb_ref[...]
        for i in range(1, X):
            x_reduce(src, other_x(i), other_x(i)).wait_recv()
            total = total + xin[src, other_x(i)].astype(F32)
        done = total.astype(BF16)
        fin[src] = done

    def finish_send(src):
        finish(src)

        @pl.when(src != s)
        def _():
            z_return(src, s).start()

        @pl.when(src == s)
        def _():
            ret[s] = fin[s]

    def chunk(k, unused):
        src = order(k)
        for i in range(1, X):
            x_forward(src, other_x(i), other_x(i)).wait_recv()
            t_forward(src, other_x(i), c).start()

        nxt = order(k + 1)
        late = (k == own_turn) & (k == 1)

        @pl.when((k + 1 < S) & (nxt != s) & jnp.logical_not(late))
        def _():
            z_copy(nxt, nxt).wait_recv()
            forward(nxt)

        for i in range(X):
            t_forward(src, other_x(i), oc).wait_recv()
        for i in range(1, X):
            x_forward(src, other_x(i), x).wait_send()
        for i in range(X):
            t_forward(src, other_x(i), c).wait_send()

        block = rows[src].reshape(2 * X * capp, D)
        hidden = jnp.dot(block, up_v[...], preferred_element_type=F32) + upb_ref[...]
        hidden = jax.nn.gelu(hidden).astype(BF16)
        result = jnp.dot(hidden, down_v[...], preferred_element_type=F32).astype(BF16)
        rows[src] = result.reshape(2, X, capp, D)
        t_reduce(src).start()

        @pl.when(k >= 1)
        def _():
            finish_send(order(k - 1))

        @pl.when((k + 1 < S) & late)
        def _():
            z_copy(nxt, nxt).wait_recv()
            forward(nxt)

        @pl.when((k >= 1) & (k < S - 1))
        def _():
            relay(k + 1)

        t_reduce(src).wait_recv()
        for i in range(X):
            to = other_x(i)
            rows[src, c, to] = (rows[src, c, to].astype(F32) + tpin[src, to].astype(F32)).astype(BF16)
            if i > 0:
                x_reduce(src, to, x).start()
        return unused

    lax.fori_loop(0, S, chunk, jnp.int32(0))

    relay(S)

    for i in range(S):
        keys_v[pl.ds(i * L, L), :] = kv[i, 0].T
    scale = 1.0 / math.sqrt(HD)
    channel = lax.broadcasted_iota(jnp.int32, (W, L), 0)

    def head(h, unused):
        mine = (channel >= h * HD) & (channel < (h + 1) * HD)
        query = jnp.where(mine, q_ref[...].astype(F32), 0.0).astype(BF16)
        scores = jnp.dot(keys_v[...], query, preferred_element_type=F32) * scale
        probs = jnp.exp(scores - jnp.max(scores, axis=0, keepdims=True))
        total = jnp.sum(probs, axis=0, keepdims=True)
        weights = probs.astype(BF16)
        mixed = jnp.zeros((W, L), F32)
        for i in range(S):
            mixed += jnp.dot(kv[i, 1], weights[i * L : (i + 1) * L], preferred_element_type=F32)
        acc[...] = jnp.where(mine, mixed / total, acc[...])
        return unused

    acc[...] = jnp.zeros_like(acc)
    lax.fori_loop(0, heads, head, jnp.int32(0))
    attn_ref[...] = acc[...].astype(BF16)
    finish_send(order(S - 1))

    base = jnp.where(named, place, 0.0) + (expert * capp).astype(F32)
    turn[...] = jnp.zeros_like(turn)
    for j in range(2):
        hit = ids_ref[j : j + 1, :] == expert
        turn[j : j + 1, :] = jnp.sum(jnp.where(hit, base, 0.0), axis=0, keepdims=True)
        turn[2 + j : 3 + j, :] = gate_ref[j : j + 1, :]
    turned = turn[...].T
    slot_lane = lax.broadcasted_iota(jnp.int32, (T, S * capp), 1).astype(F32)
    picks = [jnp.where(turned[:, j : j + 1] == slot_lane, 1.0, 0.0).astype(BF16) for j in range(2)]
    for i in range(1, S):
        z_return(s, lax.rem(s + i, S)).wait_recv()
    everything = ret[...].reshape(S * capp, D)
    moe_ref[...] = (
        jnp.dot(picks[0], everything, preferred_element_type=F32) * turned[:, 2:3]
        + jnp.dot(picks[1], everything, preferred_element_type=F32) * turned[:, 3:4]
    ).astype(BF16)

    def drain(i, unused):
        to = lax.rem(s + i, S)
        z_copy(to, s).wait_send()
        z_return(to, s).wait_send()
        return unused

    lax.fori_loop(1, S, drain, jnp.int32(0))

    def drain_chunk(i, unused):
        t_reduce(i).wait_send()
        for j in range(1, X):
            x_reduce(i, other_x(j), x).wait_send()

        @pl.when((i <= s) & (s + 1 < S))
        def _():
            kv_copy(i, 1).wait_send()

        @pl.when((i >= s) & (s - 1 >= 0))
        def _():
            kv_copy(i, -1).wait_send()

        return unused

    lax.fori_loop(0, S, drain_chunk, jnp.int32(0))


def local(
    attn_query, fresh_keys, fresh_values, stale_keys, stale_values, block_flags,
    moe_tokens, expert_ids, gate_weights, up_weight, up_bias, down_weight, down_bias,
):
    S, X = lax.axis_size("seq"), lax.axis_size("exp")
    assert lax.axis_size("tp") == 2 and up_weight.shape[0] == 1
    tokens, D = moe_tokens.shape
    length, width = attn_query.shape
    hidden = up_weight.shape[2]
    cap = 5 * tokens // (2 * S)
    capp = -(-cap // 16) * 16
    vmem = pl.BlockSpec(memory_space=pltpu.VMEM)
    smem = pl.BlockSpec(memory_space=pltpu.SMEM)
    hbm = pl.BlockSpec(memory_space=pl.ANY)
    dma = pltpu.SemaphoreType.DMA
    attn_out, moe_out = pl.pallas_call(
        functools.partial(layer_kernel, (S, X, capp)),
        out_shape=(
            jax.ShapeDtypeStruct((width, length), BF16),
            jax.ShapeDtypeStruct((tokens, D), BF16),
        ),
        in_specs=[vmem] * 5 + [smem] + [vmem] * 3 + [hbm, vmem, hbm, vmem],
        out_specs=(vmem, vmem),
        scratch_shapes=[
            pltpu.VMEM((D, hidden), BF16),
            pltpu.VMEM((hidden, D), BF16),
            pltpu.VMEM((S, tokens), F32),
            pltpu.VMEM((S, capp, D), BF16),
            pltpu.VMEM((S, 2, X, capp, D), BF16),
            pltpu.VMEM((S, X, capp, D), BF16),
            pltpu.VMEM((S, X, capp, D), BF16),
            pltpu.VMEM((S, capp, D), BF16),
            pltpu.VMEM((S, capp, D), BF16),
            pltpu.VMEM((S, 2, width, length), BF16),
            pltpu.VMEM((S * length, width), BF16),
            pltpu.VMEM((width, length), F32),
            pltpu.VMEM((128, tokens), F32),
            dma((2,)),
            dma((S,)), dma((S,)), dma((S, X)), dma((S, X)), dma((S, X)), dma((S, X)),
            dma((S,)), dma((S,)), dma((S, X)), dma((S, X)), dma((S,)), dma((S,)),
            dma((S,)), dma((S,)), dma((S,)),
        ],
        compiler_params=pltpu.CompilerParams(
            collective_id=0, has_side_effects=True, vmem_limit_bytes=67043328
        ),
    )(
        attn_query.T, fresh_keys.T, fresh_values.T, stale_keys.T, stale_values.T, block_flags,
        moe_tokens, expert_ids.T, gate_weights.T,
        up_weight, up_bias, down_weight, down_bias,
    )
    return attn_out.T, moe_out


def solution(mesh):
    in_specs = (
        P(("groups", "seq"), ("exp", "tp")),
        P(("groups", "seq"), ("exp", "tp")),
        P(("groups", "seq"), ("exp", "tp")),
        P(("groups", "seq"), ("exp", "tp")),
        P(("groups", "seq"), ("exp", "tp")),
        P(("groups", "seq")),
        P(("groups", "seq", "exp", "tp"), None),
        P(("groups", "seq", "exp", "tp"), None),
        P(("groups", "seq", "exp", "tp"), None),
        P("seq", None, ("exp", "tp")),
        P("seq", ("exp", "tp")),
        P("seq", ("exp", "tp"), None),
        P("seq", None),
    )
    out_specs = (P(("groups", "seq"), ("exp", "tp")), P(("groups", "seq", "exp", "tp"), None))
    return jax.shard_map(local, mesh=mesh, in_specs=in_specs, out_specs=out_specs, check_vma=False)
```

```python
import functools
import math

import jax
import jax.numpy as jnp
from jax import lax
from jax.experimental import pallas as pl
from jax.experimental.pallas import tpu as pltpu
from jax.sharding import PartitionSpec as P

HD = 72
MESH = pl.DeviceIdType.MESH
F32 = jnp.float32
BF16 = jnp.bfloat16


def layer_kernel(
    sizes,
    q_ref, fresh_k, fresh_v, stale_k, stale_v, flags,
    tok_ref, ids_ref, gate_ref,
    up_hbm, upb_ref, down_hbm, downb_ref,
    attn_ref, moe_ref,
    up_v, down_v, place_v, disp, rows, tpin, xin, fin, ret, kv, keys_v, acc, turn,
    w_sem,
    z_send, z_recv, xf_send, xf_recv, tf_send, tf_recv,
    tr_send, tr_recv, xr_send, xr_recv, zr_send, zr_recv, kv_right, kv_left, kv_recv,
):
    S, X, capp = sizes
    s, x, c = lax.axis_index("seq"), lax.axis_index("exp"), lax.axis_index("tp")
    oc = 1 - c
    T, D = tok_ref.shape
    W, L = q_ref.shape
    heads = W // HD
    blk = L // flags.shape[0]

    up_copy = pltpu.make_async_copy(up_hbm.at[0], up_v, w_sem.at[0])
    down_copy = pltpu.make_async_copy(down_hbm.at[0], down_v, w_sem.at[1])
    up_copy.start()
    down_copy.start()

    def rdma(src, dst, ssem, rsem, where):
        return pltpu.make_async_remote_copy(
            src_ref=src, dst_ref=dst, send_sem=ssem, recv_sem=rsem,
            device_id=where, device_id_type=MESH,
        )

    def z_copy(e, slot):
        return rdma(disp.at[e], rows.at[slot, c, x], z_send.at[e], z_recv.at[slot], {"seq": e})

    def x_forward(src, to, origin):
        return rdma(
            rows.at[src, c, origin], rows.at[src, c, origin],
            xf_send.at[src, to], xf_recv.at[src, origin], {"exp": to},
        )

    def t_forward(src, origin, side):
        return rdma(
            rows.at[src, side, origin], rows.at[src, side, origin],
            tf_send.at[src, origin], tf_recv.at[src, origin], {"tp": oc},
        )

    def t_reduce(src):
        return rdma(rows.at[src, oc], tpin.at[src], tr_send.at[src], tr_recv.at[src], {"tp": oc})

    def x_reduce(src, to, origin):
        return rdma(
            rows.at[src, c, to], xin.at[src, origin],
            xr_send.at[src, to], xr_recv.at[src, origin], {"exp": to},
        )

    def z_return(src, slot):
        return rdma(fin.at[src], ret.at[slot], zr_send.at[src], zr_recv.at[slot], {"seq": src})

    def kv_copy(b, step):
        sems = kv_right if step > 0 else kv_left
        return rdma(kv.at[b], kv.at[b], sems.at[b], kv_recv.at[b], {"seq": s + step})

    def other_x(i):
        return lax.rem(x + i, X)

    side = jnp.minimum(s, S - 1 - s)
    own_turn = jnp.maximum(1, 2 * side)

    def remote(j):
        near = j // 2 + 1
        near = jnp.where(lax.rem(j, 2) == 0, near, -near)
        far = j - side + 1
        far = jnp.where(2 * s < S, far, -far)
        return s + jnp.where(j < 2 * side, near, far)

    def order(k):
        return jnp.where(k == own_turn, s, remote(jnp.where(k > own_turn, k - 1, k)))

    barrier = pltpu.get_barrier_semaphore()
    for i in range(1, S):
        pl.semaphore_signal(barrier, inc=1, device_id={"seq": lax.rem(s + i, S)}, device_id_type=MESH)
    for i in range(1, X):
        pl.semaphore_signal(barrier, inc=1, device_id={"exp": other_x(i)}, device_id_type=MESH)
    pl.semaphore_signal(barrier, inc=1, device_id={"tp": oc}, device_id_type=MESH)

    expert = lax.broadcasted_iota(jnp.int32, (S, T), 0)
    named = (ids_ref[0:1, :] == expert) | (ids_ref[1:2, :] == expert)
    earlier = lax.broadcasted_iota(jnp.int32, (T, T), 0) < lax.broadcasted_iota(jnp.int32, (T, T), 1)
    place = jnp.dot(
        jnp.where(named, 1.0, 0.0).astype(BF16),
        jnp.where(earlier, 1.0, 0.0).astype(BF16),
        preferred_element_type=F32,
    )
    place_v[...] = jnp.where(named, place, -1.0)
    slot_rows = lax.broadcasted_iota(jnp.int32, (capp, T), 0).astype(F32)

    def slots_of(e):
        pick = jnp.where(place_v[pl.ds(e, 1), :] == slot_rows, 1.0, 0.0).astype(BF16)
        return jnp.dot(pick, tok_ref[...], preferred_element_type=F32).astype(BF16)

    def forward(src):
        for i in range(1, X):
            x_forward(src, other_x(i), x).start()
        t_forward(src, x, c).start()

    rows[s, c, x] = slots_of(s)
    pl.semaphore_wait(barrier, S - 1 + X - 1 + 1)
    forward(s)
    def dispatch(j):
        e = remote(jnp.int32(j))
        disp[e] = slots_of(e)
        z_copy(e, s).start()

    for j in range(min(2, S - 1)):
        dispatch(j)
    for b in range(flags.shape[0]):
        fresh = flags[b] == 1
        part = pl.ds(b * blk, blk)
        kv[s, 0, :, part] = jnp.where(fresh, fresh_k[:, part], stale_k[:, part])
        kv[s, 1, :, part] = jnp.where(fresh, fresh_v[:, part], stale_v[:, part])

    def relay(step):
        low, high = s - (step - 1), s + (step - 1)

        @pl.when(low >= 0)
        def _():
            @pl.when(low < s)
            def _():
                kv_copy(low, 1).wait_recv()

            @pl.when(s + 1 < S)
            def _():
                kv_copy(low, 1).start()

        @pl.when(high < S)
        def _():
            @pl.when(high > s)
            def _():
                kv_copy(high, -1).wait_recv()

            @pl.when(s - 1 >= 0)
            def _():
                kv_copy(high, -1).start()

    relay(1)
    for j in range(2, S - 1):
        dispatch(j)
    nearest = order(jnp.int32(0))
    z_copy(nearest, nearest).wait_recv()
    forward(nearest)

    up_copy.wait()
    down_copy.wait()

    def finish(src):
        total = rows[src, c, x].astype(F32) + downb_ref[...]
        for i in range(1, X):
            x_reduce(src, other_x(i), other_x(i)).wait_recv()
            total = total + xin[src, other_x(i)].astype(F32)
        done = total.astype(BF16)
        fin[src] = done

    def finish_send(src):
        finish(src)

        @pl.when(src != s)
        def _():
            z_return(src, s).start()

        @pl.when(src == s)
        def _():
            ret[s] = fin[s]

    def chunk(k, unused):
        src = order(k)
        for i in range(1, X):
            x_forward(src, other_x(i), other_x(i)).wait_recv()
            t_forward(src, other_x(i), c).start()

        nxt = order(k + 1)
        late = (k == own_turn) & (k == 1)

        @pl.when((k + 1 < S) & (nxt != s) & jnp.logical_not(late))
        def _():
            z_copy(nxt, nxt).wait_recv()
            forward(nxt)

        for i in range(X):
            t_forward(src, other_x(i), oc).wait_recv()
        for i in range(1, X):
            x_forward(src, other_x(i), x).wait_send()
        for i in range(X):
            t_forward(src, other_x(i), c).wait_send()

        block = rows[src].reshape(2 * X * capp, D)
        hidden = jnp.dot(block, up_v[...], preferred_element_type=F32) + upb_ref[...]
        hidden = jax.nn.gelu(hidden).astype(BF16)
        result = jnp.dot(hidden, down_v[...], preferred_element_type=F32).astype(BF16)
        rows[src] = result.reshape(2, X, capp, D)
        t_reduce(src).start()

        @pl.when(k >= 1)
        def _():
            finish_send(order(k - 1))

        @pl.when((k + 1 < S) & late)
        def _():
            z_copy(nxt, nxt).wait_recv()
            forward(nxt)

        @pl.when((k == 1) & (k < S - 1))
        def _():
            relay(2)

        @pl.when(k >= 3)
        def _():
            relay(k)

        t_reduce(src).wait_recv()
        for i in range(X):
            to = other_x(i)
            rows[src, c, to] = (rows[src, c, to].astype(F32) + tpin[src, to].astype(F32)).astype(BF16)
            if i > 0:
                x_reduce(src, to, x).start()
        return unused

    lax.fori_loop(0, S, chunk, jnp.int32(0))

    finish_send(order(S - 1))
    relay(S)

    for i in range(S):
        keys_v[pl.ds(i * L, L), :] = kv[i, 0].T
    scale = 1.0 / math.sqrt(HD)
    channel = lax.broadcasted_iota(jnp.int32, (W, L), 0)

    def head(h, unused):
        mine = (channel >= h * HD) & (channel < (h + 1) * HD)
        query = jnp.where(mine, q_ref[...].astype(F32), 0.0).astype(BF16)
        scores = jnp.dot(keys_v[...], query, preferred_element_type=F32) * scale
        probs = jnp.exp(scores - jnp.max(scores, axis=0, keepdims=True))
        total = jnp.sum(probs, axis=0, keepdims=True)
        weights = probs.astype(BF16)
        mixed = jnp.zeros((W, L), F32)
        for i in range(S):
            mixed += jnp.dot(kv[i, 1], weights[i * L : (i + 1) * L], preferred_element_type=F32)
        acc[...] = jnp.where(mine, mixed / total, acc[...])
        return unused

    acc[...] = jnp.zeros_like(acc)
    lax.fori_loop(0, heads, head, jnp.int32(0))
    attn_ref[...] = acc[...].astype(BF16)

    base = jnp.where(named, place, 0.0) + (expert * capp).astype(F32)
    turn[...] = jnp.zeros_like(turn)
    for j in range(2):
        hit = ids_ref[j : j + 1, :] == expert
        turn[j : j + 1, :] = jnp.sum(jnp.where(hit, base, 0.0), axis=0, keepdims=True)
        turn[2 + j : 3 + j, :] = gate_ref[j : j + 1, :]
    turned = turn[...].T
    slot_lane = lax.broadcasted_iota(jnp.int32, (T, S * capp), 1).astype(F32)
    picks = [jnp.where(turned[:, j : j + 1] == slot_lane, 1.0, 0.0).astype(BF16) for j in range(2)]
    for i in range(1, S):
        z_return(s, lax.rem(s + i, S)).wait_recv()
    everything = ret[...].reshape(S * capp, D)
    moe_ref[...] = (
        jnp.dot(picks[0], everything, preferred_element_type=F32) * turned[:, 2:3]
        + jnp.dot(picks[1], everything, preferred_element_type=F32) * turned[:, 3:4]
    ).astype(BF16)

    def drain(i, unused):
        to = lax.rem(s + i, S)
        z_copy(to, s).wait_send()
        z_return(to, s).wait_send()
        return unused

    lax.fori_loop(1, S, drain, jnp.int32(0))

    def drain_chunk(i, unused):
        t_reduce(i).wait_send()
        for j in range(1, X):
            x_reduce(i, other_x(j), x).wait_send()

        @pl.when((i <= s) & (s + 1 < S))
        def _():
            kv_copy(i, 1).wait_send()

        @pl.when((i >= s) & (s - 1 >= 0))
        def _():
            kv_copy(i, -1).wait_send()

        return unused

    lax.fori_loop(0, S, drain_chunk, jnp.int32(0))


def local(
    attn_query, fresh_keys, fresh_values, stale_keys, stale_values, block_flags,
    moe_tokens, expert_ids, gate_weights, up_weight, up_bias, down_weight, down_bias,
):
    S, X = lax.axis_size("seq"), lax.axis_size("exp")
    assert lax.axis_size("tp") == 2 and up_weight.shape[0] == 1
    tokens, D = moe_tokens.shape
    length, width = attn_query.shape
    hidden = up_weight.shape[2]
    cap = 5 * tokens // (2 * S)
    capp = -(-cap // 16) * 16
    vmem = pl.BlockSpec(memory_space=pltpu.VMEM)
    smem = pl.BlockSpec(memory_space=pltpu.SMEM)
    hbm = pl.BlockSpec(memory_space=pl.ANY)
    dma = pltpu.SemaphoreType.DMA
    attn_out, moe_out = pl.pallas_call(
        functools.partial(layer_kernel, (S, X, capp)),
        out_shape=(
            jax.ShapeDtypeStruct((width, length), BF16),
            jax.ShapeDtypeStruct((tokens, D), BF16),
        ),
        in_specs=[vmem] * 5 + [smem] + [vmem] * 3 + [hbm, vmem, hbm, vmem],
        out_specs=(vmem, vmem),
        scratch_shapes=[
            pltpu.VMEM((D, hidden), BF16),
            pltpu.VMEM((hidden, D), BF16),
            pltpu.VMEM((S, tokens), F32),
            pltpu.VMEM((S, capp, D), BF16),
            pltpu.VMEM((S, 2, X, capp, D), BF16),
            pltpu.VMEM((S, X, capp, D), BF16),
            pltpu.VMEM((S, X, capp, D), BF16),
            pltpu.VMEM((S, capp, D), BF16),
            pltpu.VMEM((S, capp, D), BF16),
            pltpu.VMEM((S, 2, width, length), BF16),
            pltpu.VMEM((S * length, width), BF16),
            pltpu.VMEM((width, length), F32),
            pltpu.VMEM((128, tokens), F32),
            dma((2,)),
            dma((S,)), dma((S,)), dma((S, X)), dma((S, X)), dma((S, X)), dma((S, X)),
            dma((S,)), dma((S,)), dma((S, X)), dma((S, X)), dma((S,)), dma((S,)),
            dma((S,)), dma((S,)), dma((S,)),
        ],
        compiler_params=pltpu.CompilerParams(
            collective_id=0, has_side_effects=True, vmem_limit_bytes=67043328
        ),
    )(
        attn_query.T, fresh_keys.T, fresh_values.T, stale_keys.T, stale_values.T, block_flags,
        moe_tokens, expert_ids.T, gate_weights.T,
        up_weight, up_bias, down_weight, down_bias,
    )
    return attn_out.T, moe_out


def solution(mesh):
    in_specs = (
        P(("groups", "seq"), ("exp", "tp")),
        P(("groups", "seq"), ("exp", "tp")),
        P(("groups", "seq"), ("exp", "tp")),
        P(("groups", "seq"), ("exp", "tp")),
        P(("groups", "seq"), ("exp", "tp")),
        P(("groups", "seq")),
        P(("groups", "seq", "exp", "tp"), None),
        P(("groups", "seq", "exp", "tp"), None),
        P(("groups", "seq", "exp", "tp"), None),
        P("seq", None, ("exp", "tp")),
        P("seq", ("exp", "tp")),
        P("seq", ("exp", "tp"), None),
        P("seq", None),
    )
    out_specs = (P(("groups", "seq"), ("exp", "tp")), P(("groups", "seq", "exp", "tp"), None))
    return jax.shard_map(local, mesh=mesh, in_specs=in_specs, out_specs=out_specs, check_vma=False)
```
